32 devices in a mesh: slab: 32 (over z, y, x, core).
Axes of the slice: x: 2, y: 2, z: 4, core: 2. Of those that a mesh axis runs over, the one named last changes fastest.
Arguments:
- start_vectors: float32 [2, 32, 256, 256], P(None, 'slab'), may hold values from -6 to 6
- levels: int32 [32, 256, 256], P('slab'), may hold values from 0 to 15
- energies: float32 [16], replicated, may hold values from -4 to 4
Outputs:
- cheb_field: float32 [2, 32, 256, 256], P(None, 'slab')
- lanczos_diag: float32 [2, 8], replicated
- lanczos_off: float32 [2, 7], replicated
- moments: float32 [2, 6], replicated
The draws below stay inside these ranges and needn't reach their ends.
All inputs are finite; a program needn't handle non-finite values.
Results may differ from the reference program's by a relative error of at most 0.0001.
Values sent between devices are 32-bit elements; how exact they have to be, the bound alone decides.
A program may use at most 64 MiB of HBM per device.

```python
import jax
import jax.numpy as jnp
from jax import lax

NY = 256
NX = 256
VECS = 2
LANCZOS = 8
LEVELS = 16
NZ = 32


def place_ends(entries, stream_key, low, largest):
    shape = entries.shape
    index_at = [jax.random.randint(jax.random.fold_in(stream_key, axis), (), 0, shape[axis]) for axis in range(len(shape))]
    entries = entries.at[tuple(index_at)].set(low)
    longest = shape.index(max(shape))
    index_at[longest] = (index_at[longest] + 1) % shape[longest]
    return entries.at[tuple(index_at)].set(largest)


def shard_levels(stream_key, shape, cuts, least, largest):
    loudness = 1.0
    for position, blocks in cuts:
        heights = jax.random.uniform(jax.random.fold_in(jax.random.fold_in(stream_key, 6), position), (blocks,), jnp.float32, least / len(cuts), largest / len(cuts))
        loudness = loudness * jnp.repeat(jnp.exp(heights), shape[position] // blocks).reshape((-1,) + (1,) * (len(shape) - 1 - position))
    return loudness


def normal_values(stream_key, extent, spread, most, shards=(), held_as=jnp.bfloat16):
    array = spread * jax.random.normal(stream_key, extent, jnp.float32)
    if shards:
        array = array * shard_levels(stream_key, extent, shards, -0.22, 0.18)
    return jnp.clip(array, -most, most).astype(held_as)


def setup_inputs(seed: int = 0) -> dict:
    arg_keys = jax.random.split(jax.random.key(seed), 4)
    return {
        "start_vectors": normal_values(arg_keys[0], (VECS, NZ, NY, NX), 1.0, 6.0, ((1, 32),), jnp.float32),
        "levels": place_ends(jax.random.randint(arg_keys[1], (NZ, NY, NX), 0, LEVELS), jax.random.fold_in(arg_keys[1], 1), 0, LEVELS - 1).astype(jnp.int32),
        "energies": jnp.clip(jax.random.uniform(arg_keys[2], (LEVELS,), jnp.float32, -4.0, 4.0), -4.0, 4.0),
    }


def hamiltonian(field, onsite):
    beside = jnp.roll(field, 1, 1) + jnp.roll(field, -1, 1)
    beside = beside + jnp.roll(field, 1, 2) + jnp.roll(field, -1, 2)
    beside = beside + jnp.roll(field, 1, 3) + jnp.roll(field, -1, 3)
    return onsite[None] * field - beside

def inner(first, second):
    return lax.optimization_barrier(jnp.sum(first * second, axis=(1, 2, 3)))

def expand(values):
    return values[:, None, None, None]

def reference(start_vectors, levels, energies):
    onsite = jnp.take(energies, levels, axis=0)
    norm0 = inner(start_vectors, start_vectors)
    vector = start_vectors / expand(jnp.sqrt(norm0))
    previous = jnp.zeros_like(vector)
    beta_prev = jnp.zeros((VECS,), jnp.float32)
    alphas = []
    betas = []
    for step in range(LANCZOS):
        work = hamiltonian(vector, onsite) - expand(beta_prev) * previous
        alpha = inner(vector, work)
        alphas.append(alpha)
        if step < LANCZOS - 1:
            work = work - expand(alpha) * vector
            beta = jnp.sqrt(inner(work, work))
            betas.append(beta)
            previous, vector, beta_prev = (vector, work / expand(beta), beta)
    diag = jnp.stack(alphas, axis=1)
    offd = jnp.stack(betas, axis=1)
    zero_col = jnp.zeros((VECS, 1), jnp.float32)
    left = jnp.concatenate([zero_col, offd], axis=1)
    right = jnp.concatenate([offd, zero_col], axis=1)
    emin = lax.optimization_barrier(jnp.min(diag - left - right, axis=1))
    emax = lax.optimization_barrier(jnp.max(diag + left + right, axis=1))
    center = expand((emax + emin) * 0.5)
    half = expand(0.55 * (emax - emin))

    def scaled(field):
        return (hamiltonian(field, onsite) - center * field) / half
    term0 = start_vectors
    term1 = scaled(term0)
    term2 = 2.0 * scaled(term1) - term0
    term3 = 2.0 * scaled(term2) - term1
    first = inner(term0, term1)
    moments = jnp.stack([first, inner(term0, term2), inner(term0, term3), 2.0 * inner(term2, term2) - norm0, 2.0 * inner(term3, term2) - first, 2.0 * inner(term3, term3) - norm0], axis=1) / norm0[:, None]
    return (term3, diag, offd, moments)
```

```python
import functools

import jax
import jax.numpy as jnp
from jax import lax
from jax.experimental import pallas as pl
from jax.experimental.pallas import tpu as pltpu
from jax.sharding import PartitionSpec as P

LANCZOS = 8
ROUNDS = LANCZOS // 2
GROUP = 8
RETURNED = 3


def lanczos(dots, steps, sqrt):
    norm = dots[0]
    inv_norm = 1.0 / norm
    nu = [None] * len(dots)
    nu[0] = norm * 0.0 + 1.0
    nu[1] = dots[1] * inv_norm
    for k in range(2, len(dots)):
        nu[k] = 2.0 * (dots[k] * inv_norm) - nu[k % 2]
    top = len(nu) - 1
    row, before = list(nu), None
    diag, offd = [], []
    for k in range(steps):
        if k == 0:
            alpha = row[1]
        else:
            alpha = (0.5 * row[k + 1] - offd[-1] * before[k]) / row[k]
        diag.append(alpha)
        if k == steps - 1:
            break
        new = [None] * len(nu)
        for l in range(k + 1, top - k):
            new[l] = 0.5 * (row[l + 1] + row[l - 1]) - alpha * row[l]
            if k:
                new[l] = new[l] - offd[-1] * before[l]
        beta = sqrt(new[k + 1] / (row[k] if k == 0 else 2.0 * row[k]))
        offd.append(beta)
        inv = 1.0 / beta
        before, row = row, [None if x is None else x * inv for x in new]
    return nu, diag, offd


def chebyshev(diag, offd, nu, centre, width):
    left = [None] + offd
    right = offd + [None]
    low, high = None, None
    for a, b, c in zip(diag, left, right):
        reach = b if c is None else c if b is None else b + c
        low = a - reach if low is None else jnp.minimum(low, a - reach)
        high = a + reach if high is None else jnp.maximum(high, a + reach)
    inv = 1.0 / (0.55 * (high - low))
    al = width * inv
    be = (centre - 0.5 * (high + low)) * inv
    p, q, r = 2.0 * be * be + al * al - 1.0, 4.0 * al * be, al * al
    first = [be, al]
    second = [p, q, r]
    third = [2.0 * be * p + al * q - be, 2.0 * be * q + al * (2.0 * p + r) - al, 2.0 * be * r + al * q, al * r]

    def dot(f, g):
        total = None
        for i, x in enumerate(f):
            for j, y in enumerate(g):
                term = (x * y) * (0.5 * (nu[i + j] + nu[abs(i - j)]))
                total = term if total is None else total + term
        return total

    start = [nu[0]]
    m1 = dot(start, first)
    moments = [
        m1,
        dot(start, second),
        dot(start, third),
        2.0 * dot(second, second) - 1.0,
        2.0 * dot(third, second) - m1,
        2.0 * dot(third, third) - 1.0,
    ]
    return third, moments


def ring_place(chip):
    return chip + lax.rem(chip // 2, 2) * (1 - 2 * lax.rem(chip, 2))


def kernel(
    count, energies, start, levels, cheb, diag_out, offd_out, moments_out,
    own, own_levels, field, twice, level, back,
    plane_in, partial_in, partial_out, edge_in, edge_out, edge, corner_in, corner_out, slots, mine,
    load_sem, vec_sem, level_in, level_sem, plane_sem, partial_sem, edge_sem, corner_sem, back_sem, sum_sem,
):
    me = lax.axis_index("slab")
    member = lax.rem(me, GROUP)
    base = me - member
    vecs, _, height, lanes = start.shape
    blocks = GROUP // vecs
    rows = height // blocks
    core, chip = lax.rem(member, vecs), member // vecs
    block = ring_place(chip)
    mesh_id = pl.DeviceIdType.MESH
    ahead_base = lax.rem(base + GROUP, count)
    behind_base = lax.rem(base + count - GROUP, count)
    above = ring_place(lax.rem(block + blocks - 1, blocks)) * vecs + core
    below = ring_place(lax.rem(block + 1, blocks)) * vecs + core
    partner = base + chip * vecs + lax.rem(core + 1, vecs)
    last = GROUP - 1

    loads = [
        pltpu.make_async_copy(start.at[:, 0], own, load_sem.at[0]),
        pltpu.make_async_copy(levels.at[0], own_levels, load_sem.at[1]),
    ]
    for copy in loads:
        copy.start()

    def remote(src, dst, send, recv, to):
        return pltpu.make_async_remote_copy(
            src_ref=src, dst_ref=dst, send_sem=send, recv_sem=recv, device_id=(to,), device_id_type=mesh_id
        )

    def drain(ref, sem):
        pltpu.make_async_copy(ref, ref, sem).wait()

    barrier = pltpu.get_barrier_semaphore()

    def greet(to):
        pl.semaphore_signal(barrier, inc=1, device_id=(to,), device_id_type=mesh_id)

    def greet_member(i, carry):
        greet(base + lax.rem(member + i, GROUP))
        return carry

    for side in (behind_base, ahead_base):
        for place in (member, above, below):
            greet(side + place)
    lax.fori_loop(1, GROUP, greet_member, 0)
    pl.semaphore_wait(barrier, GROUP - 1 + 6)

    def rows_of(at):
        return pl.ds(pl.multiple_of(at * rows, 8), rows)

    loads[0].wait()

    def scatter_vec(i, carry):
        to = lax.rem(member + i, GROUP)
        src = own.at[lax.rem(to, vecs), rows_of(ring_place(to // vecs))]
        remote(src, field.at[0, member], vec_sem.at[0], vec_sem.at[1], base + to).start()
        return carry

    lax.fori_loop(1, GROUP, scatter_vec, 0)
    pltpu.make_async_copy(own.at[core, rows_of(block)], field.at[0, member], vec_sem.at[1]).start()
    loads[1].wait()

    def scatter_level(i, carry):
        to = lax.rem(chip + i, blocks)
        src = own_levels.at[rows_of(ring_place(to))]
        remote(src, level.at[member], level_sem.at[0], level_in.at[chip], base + to * vecs + core).start()
        return carry

    lax.fori_loop(1, blocks, scatter_level, 0)
    pltpu.make_async_copy(own_levels.at[rows_of(block)], level.at[member], level_in.at[chip]).start()

    values = [energies[i] for i in range(energies.shape[0])]
    share = 1.0 / len(values)

    def total(terms):
        return sum(terms[1:], terms[0])

    mean = total(values) * share
    apart = [x - mean for x in values]
    square = [x * x for x in apart]
    second = total(square) * share + 6.0
    cube = total([x * y for x, y in zip(square, apart)]) * share
    fourth = total([x * x for x in square]) * share + 24.0 * (second - 6.0) + 90.0
    inv_second = 1.0 / jnp.full((1, lanes), second, jnp.float32)
    skew = cube * inv_second
    centre = mean + 0.5 * skew
    width = jnp.sqrt(2.0 * (fourth * inv_second - skew * skew))
    scale = 2.0 / width

    sub = lax.broadcasted_iota(jnp.int32, (8, lanes), 0)
    zero_row = jnp.zeros((1, lanes), jnp.float32)

    def look_up(m):
        ids = level[m]
        found = [jnp.full(ids.shape, x, jnp.float32) for x in values]
        bit = 1
        while len(found) > 1:
            odd = (ids & bit) != 0
            found = [
                found[i] if i + 1 == len(found) else jnp.where(odd, found[i + 1], found[i])
                for i in range(0, len(found), 2)
            ]
            bit *= 2
        twice[m] = (found[0] - centre) * scale

    def z_copies(r, k):
        return [
            remote(
                field.at[k, m], plane_in.at[r, 1 - z],
                plane_sem.at[0, r, z], plane_sem.at[1, r, 1 - z], side + member,
            )
            for z, m, side in ((0, 0, behind_base), (1, last, ahead_base))
        ]

    def q_copies(r):
        sides = ((0, behind_base), (1, ahead_base))
        return [
            remote(
                partial_out.at[r, z], partial_in.at[r, 1 - z],
                partial_sem.at[0, r, z], partial_sem.at[1, r, 1 - z], side + member,
            )
            for z, side in (sides[:1] if r == ROUNDS - 1 else sides)
        ]

    def y_copies(r, kind):
        return [
            remote(
                edge_out.at[r, kind, y], edge_in.at[r, kind, 1 - y],
                edge_sem.at[0, r, kind], edge_sem.at[1, r, kind], base + place,
            )
            for y, place in ((0, above), (1, below))
        ]

    def corner_copies(r):
        return [
            remote(
                corner_out.at[r, 2 * z + y], corner_in.at[r, 2 * (1 - z) + (1 - y)],
                corner_sem.at[0, r], corner_sem.at[1, r], side + place,
            )
            for z, side in ((0, behind_base), (1, ahead_base))
            for y, place in ((0, above), (1, below))
        ]

    def begin(copies):
        for copy in copies:
            copy.start()

    def put_corners(r, z, value):
        corner_out[r, 2 * z] = value[0:1]
        corner_out[r, 2 * z + 1] = value[rows - 1 : rows]

    def put_edges(r, kind, m, value):
        edge_out[r, kind, 0, m] = value[0:1]
        edge_out[r, kind, 1, m] = value[rows - 1 : rows]

    def around(here, top, bottom):
        up, down = pltpu.roll(here, 1, 0), pltpu.roll(here, rows - 1, 0)
        first = jnp.where(sub == 0, top, up[0:8])
        final = jnp.where(sub == 7, bottom, down[rows - 8 :])
        near = jnp.concatenate([first, up[8:]], 0) + jnp.concatenate([down[: rows - 8], final], 0)
        return near + (pltpu.roll(here, 1, 1) + pltpu.roll(here, lanes - 1, 1))

    def partial(k, m, *beside):
        here = field[k, m]
        near = around(here, zero_row, zero_row)
        for plane in beside:
            near = near + field[k, plane]
        new = twice[m] * here - scale * near
        new = 0.5 * new if k == 0 else new - field[k - 1, m]
        field[k + 1, m] = new
        return new

    def tile_sum(x):
        parts = [x[i : i + 8] for i in range(0, rows, 8)]
        while len(parts) > 1:
            parts = [a + b for a, b in zip(parts[::2], parts[1::2])]
        return parts[0]

    def follow(k, m, near, sums):
        here, old = field[k + 1, m], field[k, m]
        near = near + around(here, edge[0, m], edge[1, m])
        new = twice[m] * here - scale * near - old
        terms = [old * here, here * here, here * new]
        if k + 2 < LANCZOS:
            field[k + 2, m] = new
            put_edges(k // 2 + 1, 0, m, new)
            terms.append(new * new)
        if k == 0:
            terms.append(old * old)
        return new, tuple(a + tile_sum(b) for a, b in zip(sums, terms))

    def give_back(k):
        def body(i, carry):
            to = lax.rem(member + i, GROUP)
            remote(
                field.at[k, to], back.at[k - 1, core, rows_of(block)],
                back_sem.at[0, k - 1], back_sem.at[1, k - 1], base + to,
            ).start()
            return carry

        lax.fori_loop(1, GROUP, body, 0)
        pltpu.make_async_copy(
            field.at[k, member], back.at[k - 1, core, rows_of(block)], back_sem.at[1, k - 1]
        ).start()

    def partial_faces(r):
        k = 2 * r
        for side, (m, inner) in enumerate(((0, 1), (last, last - 1))):
            new = partial(k, m, inner)
            if r < ROUNDS - 1 or side == 0:
                partial_out[r, side] = new
            put_edges(r, 1, m, new)
        begin(q_copies(r))

    def partial_rest(r):
        def body(m, carry):
            put_edges(r, 1, m, partial(2 * r, m, m - 1, m + 1))
            return carry

        lax.fori_loop(1, last, body, 0, unroll=2)
        begin(y_copies(r, 1))

    drain(field.at[0], vec_sem.at[1])
    begin(z_copies(0, 0))

    def first_edges(m, carry):
        edge_out[0, 0, 0, m] = field[0, m, 0:1]
        edge_out[0, 0, 1, m] = field[0, m, rows - 1 : rows]
        return carry

    lax.fori_loop(0, GROUP, first_edges, 0, unroll=True)
    for z, m in ((0, 0), (1, last)):
        corner_out[0, 2 * z] = field[0, m, 0:1]
        corner_out[0, 2 * z + 1] = field[0, m, rows - 1 : rows]
    begin(y_copies(0, 0))
    begin(corner_copies(0))

    def pass_on(i, carry):
        at = lax.rem(chip + i, blocks)
        plane = at * vecs + core
        drain(level.at[plane], level_in.at[at])
        remote(level.at[plane], level.at[plane], level_sem.at[1], level_sem.at[2], partner).start()
        return carry

    lax.fori_loop(0, blocks, pass_on, 0)

    def look_up_own(i, carry):
        look_up(i * vecs + core)
        return carry

    def look_up_other(i, carry):
        look_up(i * vecs + lax.rem(core + 1, vecs))
        return carry

    lax.fori_loop(0, blocks, look_up_own, 0)
    drain(level.at[pl.ds(0, blocks)], level_sem.at[2])
    lax.fori_loop(0, blocks, look_up_other, 0)

    nothing = jnp.zeros((8, lanes), jnp.float32)
    dots = [None] * (2 * LANCZOS)
    partial_faces(0)
    partial_rest(0)
    for r in range(ROUNDS):
        k = 2 * r
        final = r == ROUNDS - 1
        weight = 0.5 * scale if k == 0 else scale

        drain(edge_in.at[r, 0], edge_sem.at[1, r, 0])

        def complete(m, carry):
            field[k + 1, m, 0:8] = field[k + 1, m, 0:8] - jnp.where(sub == 0, weight * edge_in[r, 0, 0, m], 0.0)
            field[k + 1, m, rows - 8 : rows] = field[k + 1, m, rows - 8 : rows] - jnp.where(
                sub == 7, weight * edge_in[r, 0, 1, m], 0.0
            )
            return carry

        lax.fori_loop(0, GROUP, complete, 0, unroll=2)
        for side, m in ((0, 0), (1, last)):
            drain(plane_in.at[r, side], plane_sem.at[1, r, side])
            field[k + 1, m] = field[k + 1, m] - weight * plane_in[r, side]

        drain(corner_in.at[r], corner_sem.at[1, r])
        drain(edge_in.at[r, 1], edge_sem.at[1, r, 1])
        for y in range(2):
            edge[y] = edge_in[r, 1, y] - weight * edge_out[r, 0, y]
            for z, m in ((0, 0), (1, last)):
                edge[y, m] = edge[y, m] - weight * corner_in[r, 2 * z + y]

        def outside(side, m):
            drain(partial_in.at[r, side], partial_sem.at[1, r, side])
            here = field[k, m] + jnp.concatenate(
                [
                    jnp.where(sub == 0, corner_in[r, 2 * side], 0.0),
                    jnp.zeros((rows - 16, lanes), jnp.float32),
                    jnp.where(sub == 7, corner_in[r, 2 * side + 1], 0.0),
                ],
                0,
            )
            return partial_in[r, side] - weight * here

        sums = (nothing,) * 5
        if final:
            _, sums = follow(k, 0, field[k + 1, 1], sums)
            _, sums = follow(k, last, field[k + 1, last - 1] + 2.0 * outside(1, last), sums + (nothing,) * (5 - len(sums)))
        else:
            for side, m, inner in ((0, 0, 1), (1, last, last - 1)):
                new, sums = follow(k, m, field[k + 1, inner] + outside(side, m), sums + (nothing,) * (5 - len(sums)))
                put_corners(r + 1, side, new)
            begin(z_copies(r + 1, k + 2))
            begin(corner_copies(r + 1))
        sums = sums[: 3 if final else 5 if k == 0 else 4]

        def middle(m, sums):
            return follow(k, m, field[k + 1, m - 1] + field[k + 1, m + 1], sums)[1]

        if final:
            sums = lax.fori_loop(1, last, middle, sums, unroll=2)
        else:
            sums = middle(1, sums)
            sums = middle(last - 1, sums)
            partial_faces(r + 1)
            sums = lax.fori_loop(2, last - 1, middle, sums, unroll=2)
            begin(y_copies(r + 1, 0))
            partial_rest(r + 1)
        dots[2 * k + 1 : 2 * k + 4] = sums[:3]
        if not final:
            dots[2 * k + 4] = sums[3]
            give_back(r + 1)
        if k == 0:
            dots[0] = sums[4]

    lane = lax.broadcasted_iota(jnp.int32, (1, 128), 1)
    tile = jnp.zeros((1, 128), jnp.float32)
    for d, value in enumerate(dots):
        whole = jnp.sum(jnp.sum(value, axis=0, keepdims=True), axis=1, keepdims=True)
        tile = jnp.where(lane == d, whole, tile)
    mine[...] = tile
    slots[me] = tile

    def tell(i, carry):
        remote(mine, slots.at[me], sum_sem.at[0], sum_sem.at[1], lax.rem(me + i, count)).start()
        return carry

    lax.fori_loop(1, count, tell, 0)
    drain(slots.at[pl.ds(0, count - 1)], sum_sem.at[1])
    totals = [slots[v] for v in range(vecs)]
    for i in range(vecs, count):
        totals[i % vecs] = totals[i % vecs] + slots[i]
    totals = jnp.concatenate(totals, 0)
    totals = [jnp.broadcast_to(totals[:, d : d + 1], (vecs, lanes)) for d in range(len(dots))]

    nu, diag, offd = lanczos(totals, LANCZOS, jnp.sqrt)
    diag = [width * a + centre for a in diag]
    offd = [width * b for b in offd]
    third, moments = chebyshev(diag, offd, nu, centre, width)

    for k in range(RETURNED):
        drain(back.at[k], back_sem.at[1, k])
    for v in range(vecs):
        value = third[0][v : v + 1] * own[v]
        for k in range(RETURNED):
            value = value + third[k + 1][v : v + 1] * back[k, v]
        cheb[v, 0] = value

    for ref, items in ((diag_out, diag), (offd_out, offd), (moments_out, moments)):
        at = lax.broadcasted_iota(jnp.int32, ref.shape, 1)
        value = jnp.zeros(ref.shape, jnp.float32)
        for i, item in enumerate(items):
            value = jnp.where(at == i, item[:, : ref.shape[1]], value)
        ref[...] = value

    for r in range(ROUNDS):
        for copy in z_copies(r, 2 * r) + q_copies(r):
            copy.wait_send()
        for kind in range(2):
            drain(edge_out.at[r, kind], edge_sem.at[0, r, kind])
        drain(corner_out.at[r], corner_sem.at[0, r])
    drain(field.at[0, pl.ds(0, GROUP - 1)], vec_sem.at[0])
    drain(level.at[pl.ds(0, blocks - 1)], level_sem.at[0])
    drain(level.at[pl.ds(0, blocks)], level_sem.at[1])
    for k in range(RETURNED):
        drain(field.at[k + 1, pl.ds(0, GROUP - 1)], back_sem.at[0, k])
    drain(slots.at[pl.ds(0, count - 1)], sum_sem.at[0])


def shards(count, start_vectors, levels, energies):
    vecs, _, height, lanes = start_vectors.shape
    blocks = GROUP // vecs
    rows = height // blocks
    f32 = jnp.float32
    vmem = pl.BlockSpec(memory_space=pltpu.VMEM)
    anywhere = pl.BlockSpec(memory_space=pl.ANY)
    dma = pltpu.SemaphoreType.DMA
    return pl.pallas_call(
        functools.partial(kernel, count),
        out_shape=(
            jax.ShapeDtypeStruct(start_vectors.shape, f32),
            jax.ShapeDtypeStruct((vecs, LANCZOS), f32),
            jax.ShapeDtypeStruct((vecs, LANCZOS - 1), f32),
            jax.ShapeDtypeStruct((vecs, 6), f32),
        ),
        in_specs=[pl.BlockSpec(memory_space=pltpu.SMEM), anywhere, anywhere],
        out_specs=(vmem,) * 4,
        scratch_shapes=[
            pltpu.VMEM((vecs, height, lanes), f32),
            pltpu.VMEM((height, lanes), jnp.int32),
            pltpu.VMEM((LANCZOS, GROUP, rows, lanes), f32),
            pltpu.VMEM((GROUP, rows, lanes), f32),
            pltpu.VMEM((GROUP, rows, lanes), jnp.int32),
            pltpu.VMEM((RETURNED, vecs, height, lanes), f32),
            pltpu.VMEM((ROUNDS, 2, rows, lanes), f32),
            pltpu.VMEM((ROUNDS, 2, rows, lanes), f32),
            pltpu.VMEM((ROUNDS, 2, rows, lanes), f32),
            pltpu.VMEM((ROUNDS, 2, 2, GROUP, 1, lanes), f32),
            pltpu.VMEM((ROUNDS, 2, 2, GROUP, 1, lanes), f32),
            pltpu.VMEM((2, GROUP, 1, lanes), f32),
            pltpu.VMEM((ROUNDS, 4, 1, lanes), f32),
            pltpu.VMEM((ROUNDS, 4, 1, lanes), f32),
            pltpu.VMEM((count, 1, 128), f32),
            pltpu.VMEM((1, 128), f32),
            dma((2,)),
            dma((2,)),
            dma((blocks,)),
            dma((3,)),
            dma((2, ROUNDS, 2)),
            dma((2, ROUNDS, 2)),
            dma((2, ROUNDS, 2)),
            dma((2, ROUNDS)),
            dma((2, RETURNED)),
            dma((2,)),
        ],
        compiler_params=pltpu.CompilerParams(
            collective_id=0, has_side_effects=True, vmem_limit_bytes=67043328
        ),
    )(energies, start_vectors, levels)


def solution(mesh):
    in_specs = (P(None, "slab", None, None), P("slab", None, None), P())
    out_specs = (P(None, "slab", None, None), P(), P(), P())
    return jax.shard_map(
        functools.partial(shards, mesh.shape["slab"]),
        mesh=mesh, in_specs=in_specs, out_specs=out_specs, check_vma=False,
    )
```

```python
import functools

import jax
import jax.numpy as jnp
from jax import lax
from jax.experimental import pallas as pl
from jax.experimental.pallas import tpu as pltpu
from jax.sharding import PartitionSpec as P

LANCZOS = 8
ROUNDS = LANCZOS // 2
GROUP = 8
RETURNED = 3
VMEM_BYTES = 16 * 2**20


def lanczos(dots, steps, sqrt):
    norm = dots[0]
    inv_norm = 1.0 / norm
    nu = [None] * len(dots)
    nu[0] = norm * 0.0 + 1.0
    nu[1] = dots[1] * inv_norm
    for k in range(2, len(dots)):
        nu[k] = 2.0 * (dots[k] * inv_norm) - nu[k % 2]
    top = len(nu) - 1
    row, before = list(nu), None
    diag, offd = [], []
    for k in range(steps):
        if k == 0:
            alpha = row[1]
        else:
            alpha = (0.5 * row[k + 1] - offd[-1] * before[k]) / row[k]
        diag.append(alpha)
        if k == steps - 1:
            break
        new = [None] * len(nu)
        for l in range(k + 1, top - k):
            new[l] = 0.5 * (row[l + 1] + row[l - 1]) - alpha * row[l]
            if k:
                new[l] = new[l] - offd[-1] * before[l]
        beta = sqrt(new[k + 1] / (row[k] if k == 0 else 2.0 * row[k]))
        offd.append(beta)
        inv = 1.0 / beta
        before, row = row, [None if x is None else x * inv for x in new]
    return nu, diag, offd


def chebyshev(diag, offd, nu, centre, width):
    left = [None] + offd
    right = offd + [None]
    low, high = None, None
    for a, b, c in zip(diag, left, right):
        reach = b if c is None else c if b is None else b + c
        low = a - reach if low is None else jnp.minimum(low, a - reach)
        high = a + reach if high is None else jnp.maximum(high, a + reach)
    inv = 1.0 / (0.55 * (high - low))
    al = width * inv
    be = (centre - 0.5 * (high + low)) * inv
    p, q, r = 2.0 * be * be + al * al - 1.0, 4.0 * al * be, al * al
    first = [be, al]
    second = [p, q, r]
    third = [2.0 * be * p + al * q - be, 2.0 * be * q + al * (2.0 * p + r) - al, 2.0 * be * r + al * q, al * r]

    def dot(f, g):
        total = None
        for i, x in enumerate(f):
            for j, y in enumerate(g):
                term = (x * y) * (0.5 * (nu[i + j] + nu[abs(i - j)]))
                total = term if total is None else total + term
        return total

    start = [nu[0]]
    m1 = dot(start, first)
    moments = [
        m1,
        dot(start, second),
        dot(start, third),
        2.0 * dot(second, second) - 1.0,
        2.0 * dot(third, second) - m1,
        2.0 * dot(third, third) - 1.0,
    ]
    return third, moments


CORES = 2


def ring_place(member):
    chip = member // CORES
    return (chip + lax.rem(chip // 2, 2) * (1 - 2 * lax.rem(chip, 2))) * CORES + lax.rem(member, CORES)


def kernel(
    count, energies, start, levels, own, back, small,
    own_energies, own_levels, field, twice, level,
    plane_in, partial_in, partial_out, edge_in, edge_out, edge, corner_in, corner_out, slots, mine,
    load_sem, vec_sem, level_sem, plane_sem, partial_sem, edge_sem, corner_sem, back_sem, sum_sem,
):
    me = lax.axis_index("slab")
    member = lax.rem(me, GROUP)
    base = me - member
    vecs, _, height, lanes = start.shape
    rows = height // GROUP
    block = ring_place(member)
    mesh_id = pl.DeviceIdType.MESH
    ahead_base = lax.rem(base + GROUP, count)
    behind_base = lax.rem(base + count - GROUP, count)
    above = ring_place(lax.rem(block + GROUP - 1, GROUP))
    below = ring_place(lax.rem(block + 1, GROUP))
    last = GROUP - 1

    loads = [pltpu.make_async_copy(start.at[v, 0], own.at[v], load_sem.at[v]) for v in range(vecs)]
    loads.append(pltpu.make_async_copy(levels.at[0], own_levels, load_sem.at[vecs]))
    loads.append(pltpu.make_async_copy(energies, own_energies, load_sem.at[vecs + 1]))
    for copy in loads:
        copy.start()

    def remote(src, dst, send, recv, to):
        return pltpu.make_async_remote_copy(
            src_ref=src, dst_ref=dst, send_sem=send, recv_sem=recv, device_id=(to,), device_id_type=mesh_id
        )

    def drain(ref, sem):
        pltpu.make_async_copy(ref, ref, sem).wait()

    barrier = pltpu.get_barrier_semaphore()

    def greet(to):
        pl.semaphore_signal(barrier, inc=1, device_id=(to,), device_id_type=mesh_id)

    def greet_member(i, carry):
        greet(base + lax.rem(member + i, GROUP))
        return carry

    greet(behind_base + member)
    greet(ahead_base + member)
    lax.fori_loop(1, GROUP, greet_member, 0)
    pl.semaphore_wait(barrier, GROUP - 1 + 2)

    def rows_of(at):
        return pl.ds(pl.multiple_of(at * rows, 8), rows)

    def scatter(src, dst, sem):
        def body(i, carry):
            to = lax.rem(member + i, GROUP)
            remote(src.at[rows_of(ring_place(to))], dst.at[member], sem.at[0], sem.at[1], base + to).start()
            return carry

        lax.fori_loop(1, GROUP, body, 0)
        pltpu.make_async_copy(src.at[rows_of(block)], dst.at[member], sem.at[1]).start()

    for v in range(vecs):
        loads[v].wait()
        scatter(own.at[v], field.at[v, 0], vec_sem.at[v])
        if v == 0:
            loads[vecs].wait()
            scatter(own_levels, level, level_sem)

    loads[vecs + 1].wait()
    values = [own_energies[i] for i in range(energies.shape[0])]
    share = 1.0 / len(values)

    def total(terms):
        return sum(terms[1:], terms[0])

    mean = total(values) * share
    apart = [x - mean for x in values]
    square = [x * x for x in apart]
    second = total(square) * share + 6.0
    cube = total([x * y for x, y in zip(square, apart)]) * share
    fourth = total([x * x for x in square]) * share + 24.0 * (second - 6.0) + 90.0
    inv_second = 1.0 / jnp.full((1, lanes), second, jnp.float32)
    skew = cube * inv_second
    centre = mean + 0.5 * skew
    width = jnp.sqrt(2.0 * (fourth * inv_second - skew * skew))
    scale = 2.0 / width

    sub = lax.broadcasted_iota(jnp.int32, (8, lanes), 0)
    zero_row = jnp.zeros((1, lanes), jnp.float32)

    def look_up(m, carry):
        ids = level[m]
        found = [jnp.full(ids.shape, x, jnp.float32) for x in values]
        bit = 1
        while len(found) > 1:
            odd = (ids & bit) != 0
            found = [
                found[i] if i + 1 == len(found) else jnp.where(odd, found[i + 1], found[i])
                for i in range(0, len(found), 2)
            ]
            bit *= 2
        twice[m] = (found[0] - centre) * scale
        return carry

    def z_copies(v, r):
        return [
            remote(
                field.at[v, 2 * r, m], plane_in.at[v, r, 1 - z],
                plane_sem.at[0, v, r, z], plane_sem.at[1, v, r, 1 - z], side + member,
            )
            for z, m, side in ((0, 0, behind_base), (1, last, ahead_base))
        ]

    def q_copies(v, r):
        sides = ((0, behind_base), (1, ahead_base))
        return [
            remote(
                partial_out.at[v, r, z], partial_in.at[v, r, 1 - z],
                partial_sem.at[0, v, r, z], partial_sem.at[1, v, r, 1 - z], side + member,
            )
            for z, side in (sides[:1] if r == ROUNDS - 1 else sides)
        ]

    def y_copies(v, r, kind):
        return [
            remote(
                edge_out.at[v, r, kind, y], edge_in.at[v, r, kind, 1 - y],
                edge_sem.at[0, v, r, kind], edge_sem.at[1, v, r, kind], base + place,
            )
            for y, place in ((0, above), (1, below))
        ]

    def corner_copies(v, r):
        return [
            remote(
                corner_out.at[v, r, 2 * z + y], corner_in.at[v, r, 2 * (1 - z) + (1 - y)],
                corner_sem.at[0, v, r], corner_sem.at[1, v, r], side + place,
            )
            for z, side in ((0, behind_base), (1, ahead_base))
            for y, place in ((0, above), (1, below))
        ]

    def begin(copies):
        for copy in copies:
            copy.start()

    def put_corners(v, r, z, value):
        corner_out[v, r, 2 * z] = value[0:1]
        corner_out[v, r, 2 * z + 1] = value[rows - 1 : rows]

    def put_edges(v, r, kind, m, value):
        edge_out[v, r, kind, 0, m] = value[0:1]
        edge_out[v, r, kind, 1, m] = value[rows - 1 : rows]

    def around(here, top, bottom):
        up, down = pltpu.roll(here, 1, 0), pltpu.roll(here, rows - 1, 0)
        first = jnp.where(sub == 0, top, up[0:8])
        final = jnp.where(sub == 7, bottom, down[rows - 8 :])
        near = jnp.concatenate([first, up[8:]], 0) + jnp.concatenate([down[: rows - 8], final], 0)
        return near + (pltpu.roll(here, 1, 1) + pltpu.roll(here, lanes - 1, 1))

    def partial(v, k, m, *beside):
        here = field[v, k, m]
        near = around(here, zero_row, zero_row)
        for plane in beside:
            near = near + field[v, k, plane]
        new = twice[m] * here - scale * near
        new = 0.5 * new if k == 0 else new - field[v, k - 1, m]
        field[v, k + 1, m] = new
        return new

    def tile_sum(x):
        parts = [x[i : i + 8] for i in range(0, rows, 8)]
        while len(parts) > 1:
            parts = [a + b for a, b in zip(parts[::2], parts[1::2])]
        return parts[0]

    def follow(v, k, m, near, sums):
        here, old = field[v, k + 1, m], field[v, k, m]
        near = near + around(here, edge[0, m], edge[1, m])
        new = twice[m] * here - scale * near - old
        terms = [old * here, here * here, here * new]
        if k + 2 < LANCZOS:
            field[v, k + 2, m] = new
            put_edges(v, k // 2 + 1, 0, m, new)
            terms.append(new * new)
        if k == 0:
            terms.append(old * old)
        return new, tuple(a + tile_sum(b) for a, b in zip(sums, terms))

    def give_back(v, k):
        send, recv = back_sem.at[0, v, k - 1], back_sem.at[1, v, k - 1]

        def body(i, carry):
            to = lax.rem(member + i, GROUP)
            remote(field.at[v, k, to], back.at[k - 1, v, rows_of(block)], send, recv, base + to).start()
            return carry

        lax.fori_loop(1, GROUP, body, 0)
        pltpu.make_async_copy(field.at[v, k, member], back.at[k - 1, v, rows_of(block)], recv).start()

    def partial_faces(v, r):
        for side, (m, inner) in enumerate(((0, 1), (last, last - 1))):
            new = partial(v, 2 * r, m, inner)
            if r < ROUNDS - 1 or side == 0:
                partial_out[v, r, side] = new
            put_edges(v, r, 1, m, new)
        begin(q_copies(v, r))

    def partial_rest(v, r):
        def body(m, carry):
            put_edges(v, r, 1, m, partial(v, 2 * r, m, m - 1, m + 1))
            return carry

        lax.fori_loop(1, last, body, 0, unroll=2)
        begin(y_copies(v, r, 1))

    def arrive(v):
        drain(field.at[v, 0], vec_sem.at[v, 1])
        for z, m in ((0, 0), (1, last)):
            corner_out[v, 0, 2 * z] = field[v, 0, m, 0:1]
            corner_out[v, 0, 2 * z + 1] = field[v, 0, m, rows - 1 : rows]
        begin(corner_copies(v, 0))
        begin(z_copies(v, 0))

        def edges(m, carry):
            edge_out[v, 0, 0, 0, m] = field[v, 0, m, 0:1]
            edge_out[v, 0, 0, 1, m] = field[v, 0, m, rows - 1 : rows]
            return carry

        lax.fori_loop(0, GROUP, edges, 0, unroll=True)
        begin(y_copies(v, 0, 0))

    nothing = jnp.zeros((8, lanes), jnp.float32)
    dots = [[None] * (2 * LANCZOS) for v in range(vecs)]

    def advance(v, r):
        k = 2 * r
        final = r == ROUNDS - 1
        weight = 0.5 * scale if k == 0 else scale

        drain(edge_in.at[v, r, 0], edge_sem.at[1, v, r, 0])

        def complete(m, carry):
            field[v, k + 1, m, 0:8] = field[v, k + 1, m, 0:8] - jnp.where(
                sub == 0, weight * edge_in[v, r, 0, 0, m], 0.0
            )
            field[v, k + 1, m, rows - 8 : rows] = field[v, k + 1, m, rows - 8 : rows] - jnp.where(
                sub == 7, weight * edge_in[v, r, 0, 1, m], 0.0
            )
            return carry

        lax.fori_loop(0, GROUP, complete, 0, unroll=2)
        for side, m in ((0, 0), (1, last)):
            drain(plane_in.at[v, r, side], plane_sem.at[1, v, r, side])
            field[v, k + 1, m] = field[v, k + 1, m] - weight * plane_in[v, r, side]
        if r == 0:
            give_back(v, 1)

        drain(edge_in.at[v, r, 1], edge_sem.at[1, v, r, 1])
        if r in (1, 2):
            give_back(v, r + 1)
        for y in range(2):
            edge[y] = edge_in[v, r, 1, y] - weight * edge_out[v, r, 0, y]

        def outside(side, m):
            drain(partial_in.at[v, r, side], partial_sem.at[1, v, r, side])
            here = field[v, k, m] + jnp.concatenate(
                [
                    jnp.where(sub == 0, corner_in[v, r, 2 * side], 0.0),
                    jnp.zeros((rows - 16, lanes), jnp.float32),
                    jnp.where(sub == 7, corner_in[v, r, 2 * side + 1], 0.0),
                ],
                0,
            )
            return partial_in[v, r, side] - weight * here

        def middle(m, sums):
            return follow(v, k, m, field[v, k + 1, m - 1] + field[v, k + 1, m + 1], sums)[1]

        sums = (nothing,) * (3 if final else 5 if k == 0 else 4)
        sums = lax.fori_loop(1, last, middle, sums, unroll=2)
        drain(corner_in.at[v, r], corner_sem.at[1, v, r])
        for y in range(2):
            for z, m in ((0, 0), (1, last)):
                edge[y, m] = edge[y, m] - weight * corner_in[v, r, 2 * z + y]
        if final:
            _, sums = follow(v, k, 0, field[v, k + 1, 1], sums)
            _, sums = follow(v, k, last, field[v, k + 1, last - 1] + 2.0 * outside(1, last), sums)
        else:
            for side, m, inner in ((0, 0, 1), (1, last, last - 1)):
                new, sums = follow(v, k, m, field[v, k + 1, inner] + outside(side, m), sums)
                put_corners(v, r + 1, side, new)
            begin(corner_copies(v, r + 1))
            begin(z_copies(v, r + 1))
            begin(y_copies(v, r + 1, 0))
            partial_faces(v, r + 1)
            partial_rest(v, r + 1)
        dots[v][2 * k + 1 : 2 * k + 4] = sums[:3]
        if not final:
            dots[v][2 * k + 4] = sums[3]
        if k == 0:
            dots[v][0] = sums[4]

    arrive(0)
    drain(level, level_sem.at[1])
    lax.fori_loop(0, GROUP, look_up, 0)
    for v in range(vecs):
        if v:
            arrive(v)
        partial_faces(v, 0)
        partial_rest(v, 0)
    for r in range(ROUNDS):
        for v in range(vecs):
            advance(v, r)

    lane = lax.broadcasted_iota(jnp.int32, (1, 128), 1)
    tile = jnp.zeros((1, 128), jnp.float32)
    for v in range(vecs):
        for d, value in enumerate(dots[v]):
            whole = jnp.sum(jnp.sum(value, axis=0, keepdims=True), axis=1, keepdims=True)
            tile = jnp.where(lane == v * len(dots[v]) + d, whole, tile)
    mine[...] = tile
    slots[me] = tile

    def tell(i, carry):
        remote(mine, slots.at[me], sum_sem.at[0], sum_sem.at[1], lax.rem(me + i, count)).start()
        return carry

    lax.fori_loop(1, count, tell, 0)
    drain(slots.at[pl.ds(0, count - 1)], sum_sem.at[1])
    parts = [slots[i] for i in range(count)]
    while len(parts) > 1:
        parts = [a + b for a, b in zip(parts[::2], parts[1::2])] + parts[len(parts) // 2 * 2 :]

    def spread(d):
        at = [v * 2 * LANCZOS + d for v in range(vecs)]
        return jnp.concatenate([jnp.broadcast_to(parts[0][:, i : i + 1], (1, 128)) for i in at], 0)

    nu, diag, offd = lanczos([spread(d) for d in range(2 * LANCZOS)], LANCZOS, jnp.sqrt)
    centre, width = centre[:, :128], width[:, :128]
    diag = [width * a + centre for a in diag]
    offd = [width * b for b in offd]
    third, moments = chebyshev(diag, offd, nu, centre, width)

    at = lax.broadcasted_iota(jnp.int32, small.shape[1:], 1)
    for n, items in enumerate((third, diag, offd, moments)):
        value = jnp.zeros(small.shape[1:], jnp.float32)
        for i, item in enumerate(items):
            value = jnp.where(at == i, item, value)
        small[n] = value

    for v in range(vecs):
        for k in range(RETURNED):
            drain(back.at[k, v], back_sem.at[1, v, k])
            drain(field.at[v, k + 1, pl.ds(0, GROUP - 1)], back_sem.at[0, v, k])
        for r in range(ROUNDS):
            for copy in z_copies(v, r) + q_copies(v, r):
                copy.wait_send()
            for kind in range(2):
                drain(edge_out.at[v, r, kind], edge_sem.at[0, v, r, kind])
            drain(corner_out.at[v, r], corner_sem.at[0, v, r])
        drain(field.at[v, 0, pl.ds(0, GROUP - 1)], vec_sem.at[v, 0])
    drain(level.at[pl.ds(0, GROUP - 1)], level_sem.at[0])
    drain(slots.at[pl.ds(0, count - 1)], sum_sem.at[0])


def finish(own, back, small, cheb, diag, offd, moments):
    vecs, lanes = own.shape[0], own.shape[2]
    for v in range(vecs):
        third = [jnp.broadcast_to(small[0, v : v + 1, k : k + 1], (1, lanes)) for k in range(RETURNED + 1)]
        value = third[0] * own[v]
        for k in range(RETURNED):
            value = value + third[k + 1] * back[k, v]
        cheb[v, 0] = value
    for n, ref in enumerate((diag, offd, moments)):
        ref[...] = small[n + 1, :, : ref.shape[1]]


def shards(count, start_vectors, levels, energies):
    vecs, _, height, lanes = start_vectors.shape
    rows = height // GROUP
    f32 = jnp.float32
    vmem = pl.BlockSpec(memory_space=pltpu.VMEM)
    dma = pltpu.SemaphoreType.DMA
    kept = pl.pallas_call(
        functools.partial(kernel, count),
        out_shape=(
            jax.ShapeDtypeStruct((vecs, height, lanes), f32),
            jax.ShapeDtypeStruct((RETURNED, vecs, height, lanes), f32),
            jax.ShapeDtypeStruct((4, vecs, 128), f32),
        ),
        in_specs=[pl.BlockSpec(memory_space=pltpu.HBM)] * 3,
        out_specs=(vmem,) * 3,
        scratch_shapes=[
            pltpu.SMEM(energies.shape, f32),
            pltpu.VMEM((height, lanes), jnp.int32),
            pltpu.VMEM((vecs, LANCZOS, GROUP, rows, lanes), f32),
            pltpu.VMEM((GROUP, rows, lanes), f32),
            pltpu.VMEM((GROUP, rows, lanes), jnp.int32),
            pltpu.VMEM((vecs, ROUNDS, 2, rows, lanes), f32),
            pltpu.VMEM((vecs, ROUNDS, 2, rows, lanes), f32),
            pltpu.VMEM((vecs, ROUNDS, 2, rows, lanes), f32),
            pltpu.VMEM((vecs, ROUNDS, 2, 2, GROUP, 1, lanes), f32),
            pltpu.VMEM((vecs, ROUNDS, 2, 2, GROUP, 1, lanes), f32),
            pltpu.VMEM((2, GROUP, 1, lanes), f32),
            pltpu.VMEM((vecs, ROUNDS, 4, 1, lanes), f32),
            pltpu.VMEM((vecs, ROUNDS, 4, 1, lanes), f32),
            pltpu.VMEM((count, 1, 128), f32),
            pltpu.VMEM((1, 128), f32),
            dma((vecs + 2,)),
            dma((vecs, 2)),
            dma((2,)),
            dma((2, vecs, ROUNDS, 2)),
            dma((2, vecs, ROUNDS, 2)),
            dma((2, vecs, ROUNDS, 2)),
            dma((2, vecs, ROUNDS)),
            dma((2, vecs, RETURNED)),
            dma((2,)),
        ],
        compiler_params=pltpu.CompilerParams(
            collective_id=0, has_side_effects=True, vmem_limit_bytes=VMEM_BYTES
        ),
    )(*(pltpu.with_memory_space_constraint(x, pltpu.HBM) for x in (energies, start_vectors, levels)))
    return pl.pallas_call(
        finish,
        out_shape=(
            jax.ShapeDtypeStruct(start_vectors.shape, f32),
            jax.ShapeDtypeStruct((vecs, LANCZOS), f32),
            jax.ShapeDtypeStruct((vecs, LANCZOS - 1), f32),
            jax.ShapeDtypeStruct((vecs, 6), f32),
        ),
        in_specs=[vmem] * 3,
        out_specs=(vmem,) * 4,
        compiler_params=pltpu.CompilerParams(vmem_limit_bytes=VMEM_BYTES),
    )(*kept)


def solution(mesh):
    in_specs = (P(None, "slab", None, None), P("slab", None, None), P())
    out_specs = (P(None, "slab", None, None), P(), P(), P())
    return jax.shard_map(
        functools.partial(shards, mesh.shape["slab"]),
        mesh=mesh, in_specs=in_specs, out_specs=out_specs, check_vma=False,
    )
```

```python
import functools

import jax
import jax.numpy as jnp
from jax import lax
from jax.experimental import pallas as pl
from jax.experimental.pallas import tpu as pltpu
from jax.sharding import PartitionSpec as P

LANCZOS = 8
ROUNDS = LANCZOS // 2
GROUP = 8
RETURNED = 3
VMEM_BYTES = 16 * 2**20


def lanczos(dots, steps, sqrt):
    inv_norm = 1.0 / dots[0]
    nu = [dots[0] * 0.0 + 1.0, dots[1] * inv_norm]
    for k in range(2, len(dots)):
        nu.append(2.0 * (dots[k] * inv_norm) - nu[k % 2])
    row, before = dict(enumerate(nu)), None
    diag, offd = [], []
    for k in range(steps):
        factor = 1.0 if k == 1 else 0.5
        alpha = row[1] if k == 0 else 0.5 * row[k + 1] - factor * before[k]
        diag.append(alpha)
        if k == steps - 1:
            break
        new = {}
        for l in range(k + 1, 2 * steps - 1 - k):
            new[l] = 0.5 * (row[l + 1] + (row[l - 1] if l - 1 > k else 1.0)) - alpha * row[l]
            if k:
                new[l] = new[l] - factor * before[l]
        first = new.pop(k + 1)
        offd.append(sqrt(first if k == 0 else 0.5 * first))
        inv = 1.0 / first
        before, row = row, {l: x * inv for l, x in new.items()}
    return nu, diag, offd


def chebyshev(diag, offd, nu, centre, width):
    left = [None] + offd
    right = offd + [None]
    low, high = None, None
    for a, b, c in zip(diag, left, right):
        reach = b if c is None else c if b is None else b + c
        low = a - reach if low is None else jnp.minimum(low, a - reach)
        high = a + reach if high is None else jnp.maximum(high, a + reach)
    inv = 1.0 / (0.55 * (high - low))
    al = width * inv
    be = (centre - 0.5 * (high + low)) * inv
    p, q, r = 2.0 * be * be + al * al - 1.0, 4.0 * al * be, al * al
    first = [be, al]
    second = [p, q, r]
    third = [2.0 * be * p + al * q - be, 2.0 * be * q + al * (2.0 * p + r) - al, 2.0 * be * r + al * q, al * r]

    def dot(f, g):
        total = None
        for i, x in enumerate(f):
            for j, y in enumerate(g):
                term = (x * y) * (0.5 * (nu[i + j] + nu[abs(i - j)]))
                total = term if total is None else total + term
        return total

    start = [nu[0]]
    m1 = dot(start, first)
    moments = [
        m1,
        dot(start, second),
        dot(start, third),
        2.0 * dot(second, second) - 1.0,
        2.0 * dot(third, second) - m1,
        2.0 * dot(third, third) - 1.0,
    ]
    return third, moments


CORES = 2


def ring_place(member):
    chip = member // CORES
    return (chip + lax.rem(chip // 2, 2) * (1 - 2 * lax.rem(chip, 2))) * CORES + lax.rem(member, CORES)


def kernel(
    count, energies, start, levels, own, back, small,
    own_energies, own_levels, field, twice, level,
    plane_in, partial_in, partial_out, edge_in, edge_out, edge, corner_in, corner_out, slots, mine,
    load_sem, vec_sem, level_sem, plane_sem, partial_sem, edge_sem, corner_sem, back_sem, sum_sem, sent,
):
    me = lax.axis_index("slab")
    member = lax.rem(me, GROUP)
    base = me - member
    vecs, _, height, lanes = start.shape
    rows = height // GROUP
    block = ring_place(member)
    mesh_id = pl.DeviceIdType.MESH
    ahead_base = lax.rem(base + GROUP, count)
    behind_base = lax.rem(base + count - GROUP, count)
    above = ring_place(lax.rem(block + GROUP - 1, GROUP))
    below = ring_place(lax.rem(block + 1, GROUP))
    last = GROUP - 1

    loads = [pltpu.make_async_copy(start.at[v, 0], own.at[v], load_sem.at[v]) for v in range(vecs)]
    loads.append(pltpu.make_async_copy(levels.at[0], own_levels, load_sem.at[vecs]))
    loads.append(pltpu.make_async_copy(energies, own_energies, load_sem.at[vecs + 1]))
    for copy in loads:
        copy.start()

    def remote(src, dst, send, recv, to):
        return pltpu.make_async_remote_copy(
            src_ref=src, dst_ref=dst, send_sem=send, recv_sem=recv, device_id=(to,), device_id_type=mesh_id
        )

    def drain(ref, sem):
        pltpu.make_async_copy(ref, ref, sem).wait()

    barrier = pltpu.get_barrier_semaphore()

    def greet(to):
        pl.semaphore_signal(barrier, inc=1, device_id=(to,), device_id_type=mesh_id)

    def greet_member(i, carry):
        greet(base + lax.rem(member + i, GROUP))
        return carry

    greet(behind_base + member)
    greet(ahead_base + member)
    lax.fori_loop(1, GROUP, greet_member, 0)
    pl.semaphore_wait(barrier, GROUP - 1 + 2)

    def rows_of(at):
        return pl.ds(pl.multiple_of(at * rows, 8), rows)

    def scatter(src, dst, send, recv):
        def body(i, carry):
            to = lax.rem(member + i, GROUP)
            remote(src.at[rows_of(ring_place(to))], dst.at[member], send, recv, base + to).start()
            return carry

        lax.fori_loop(1, GROUP, body, 0)
        pltpu.make_async_copy(src.at[rows_of(block)], dst.at[member], recv).start()

    for v in range(vecs):
        loads[v].wait()
        scatter(own.at[v], field.at[v, 0], sent.at[4], vec_sem.at[v])
        if v == 0:
            loads[vecs].wait()
            scatter(own_levels, level, sent.at[5], level_sem)

    loads[vecs + 1].wait()
    values = [own_energies[i] for i in range(energies.shape[0])]
    share = 1.0 / len(values)

    def total(terms):
        return sum(terms[1:], terms[0])

    mean = total(values) * share
    apart = [x - mean for x in values]
    square = [x * x for x in apart]
    second = total(square) * share + 6.0
    cube = total([x * y for x, y in zip(square, apart)]) * share
    fourth = total([x * x for x in square]) * share + 24.0 * (second - 6.0) + 90.0
    inv_second = 1.0 / jnp.full((1, lanes), second, jnp.float32)
    skew = cube * inv_second
    centre = mean + 0.5 * skew
    width = jnp.sqrt(2.0 * (fourth * inv_second - skew * skew))
    scale = 2.0 / width

    sub = lax.broadcasted_iota(jnp.int32, (8, lanes), 0)
    zero_row = jnp.zeros((1, lanes), jnp.float32)

    def look_up(m, carry):
        ids = level[m]
        found = [jnp.full(ids.shape, x, jnp.float32) for x in values]
        bit = 1
        while len(found) > 1:
            odd = (ids & bit) != 0
            found = [
                found[i] if i + 1 == len(found) else jnp.where(odd, found[i + 1], found[i])
                for i in range(0, len(found), 2)
            ]
            bit *= 2
        twice[m] = (found[0] - centre) * scale
        return carry

    def sides():
        flip = me // (count - GROUP)
        return ((flip, jnp.where(flip == 1, ahead_base, behind_base)), (1 - flip, jnp.where(flip == 1, behind_base, ahead_base)))

    def z_copies(v, r):
        return [
            remote(
                field.at[v, 2 * r, z * last], plane_in.at[v, r, 1 - z],
                sent.at[0], plane_sem.at[v, r % 2], side + member,
            )
            for z, side in sides()
        ]

    def q_copies(v, r):
        return [
            remote(
                partial_out.at[v, r, z], partial_in.at[v, r, 1 - z],
                sent.at[1], partial_sem.at[v, r % 2], side + member,
            )
            for z, side in (((0, behind_base),) if r == ROUNDS - 1 else sides())
        ]

    def y_copies(v, r, kind):
        return [
            remote(
                edge_out.at[v, r, kind, y], edge_in.at[v, r, kind, 1 - y],
                sent.at[2], edge_sem.at[v, r % 2, kind], base + place,
            )
            for y, place in ((0, above), (1, below))
        ]

    def corner_copies(v, r):
        return [
            remote(
                corner_out.at[v, r, 2 * z + y], corner_in.at[v, r, 2 * (1 - z) + (1 - y)],
                sent.at[3], corner_sem.at[v, r % 2], side + place,
            )
            for z, side in ((0, behind_base), (1, ahead_base))
            for y, place in ((0, above), (1, below))
        ]

    def begin(copies):
        for copy in copies:
            copy.start()

    def put_corners(v, r, z, value):
        corner_out[v, r, 2 * z] = value[0:1]
        corner_out[v, r, 2 * z + 1] = value[rows - 1 : rows]

    def put_edges(v, r, kind, m, value):
        edge_out[v, r, kind, 0, m] = value[0:1]
        edge_out[v, r, kind, 1, m] = value[rows - 1 : rows]

    def around(here, top, bottom):
        up, down = pltpu.roll(here, 1, 0), pltpu.roll(here, rows - 1, 0)
        first = jnp.where(sub == 0, top, up[0:8])
        final = jnp.where(sub == 7, bottom, down[rows - 8 :])
        near = jnp.concatenate([first, up[8:]], 0) + jnp.concatenate([down[: rows - 8], final], 0)
        return near + (pltpu.roll(here, 1, 1) + pltpu.roll(here, lanes - 1, 1))

    def partial(v, k, m, *beside):
        here = field[v, k, m]
        near = around(here, zero_row, zero_row)
        for plane in beside:
            near = near + field[v, k, plane]
        new = twice[m] * here - scale * near
        new = 0.5 * new if k == 0 else new - field[v, k - 1, m]
        field[v, k + 1, m] = new
        return new

    def tile_sum(x):
        parts = [x[i : i + 8] for i in range(0, rows, 8)]
        while len(parts) > 1:
            parts = [a + b for a, b in zip(parts[::2], parts[1::2])]
        return parts[0]

    def follow(v, k, m, near, sums):
        here, old = field[v, k + 1, m], field[v, k, m]
        near = near + around(here, edge[0, m], edge[1, m])
        new = twice[m] * here - scale * near - old
        terms = [old * here, here * here, here * new]
        if k + 2 < LANCZOS:
            field[v, k + 2, m] = new
            put_edges(v, k // 2 + 1, 0, m, new)
            terms.append(new * new)
        if k == 0:
            terms.append(old * old)
        return new, tuple(a + tile_sum(b) for a, b in zip(sums, terms))

    def give_back(v, k):
        def body(i, carry):
            to = lax.rem(member + i, GROUP)
            remote(field.at[v, k, to], back.at[k - 1, v, rows_of(block)], sent.at[6], back_sem, base + to).start()
            return carry

        lax.fori_loop(1, GROUP, body, 0)
        pltpu.make_async_copy(field.at[v, k, member], back.at[k - 1, v, rows_of(block)], back_sem).start()

    def partial_faces(v, r):
        for side, (m, inner) in enumerate(((0, 1), (last, last - 1))):
            new = partial(v, 2 * r, m, inner)
            if r < ROUNDS - 1 or side == 0:
                partial_out[v, r, side] = new
            put_edges(v, r, 1, m, new)
        begin(q_copies(v, r))

    def partial_rest(v, r):
        def body(m, carry):
            put_edges(v, r, 1, m, partial(v, 2 * r, m, m - 1, m + 1))
            return carry

        lax.fori_loop(1, last, body, 0, unroll=2)
        begin(y_copies(v, r, 1))

    def arrive(v):
        drain(field.at[v, 0], vec_sem.at[v])
        for z, m in ((0, 0), (1, last)):
            corner_out[v, 0, 2 * z] = field[v, 0, m, 0:1]
            corner_out[v, 0, 2 * z + 1] = field[v, 0, m, rows - 1 : rows]
        begin(corner_copies(v, 0))
        begin(z_copies(v, 0))

        def edges(m, carry):
            edge_out[v, 0, 0, 0, m] = field[v, 0, m, 0:1]
            edge_out[v, 0, 0, 1, m] = field[v, 0, m, rows - 1 : rows]
            return carry

        lax.fori_loop(0, GROUP, edges, 0, unroll=True)
        begin(y_copies(v, 0, 0))

    nothing = jnp.zeros((8, lanes), jnp.float32)
    dots = [[None] * (2 * LANCZOS) for v in range(vecs)]

    def advance(v, r):
        k = 2 * r
        final = r == ROUNDS - 1
        weight = 0.5 * scale if k == 0 else scale

        drain(edge_in.at[v, r, 0], edge_sem.at[v, r % 2, 0])

        def complete(m, carry):
            field[v, k + 1, m, 0:8] = field[v, k + 1, m, 0:8] - jnp.where(
                sub == 0, weight * edge_in[v, r, 0, 0, m], 0.0
            )
            field[v, k + 1, m, rows - 8 : rows] = field[v, k + 1, m, rows - 8 : rows] - jnp.where(
                sub == 7, weight * edge_in[v, r, 0, 1, m], 0.0
            )
            return carry

        lax.fori_loop(0, GROUP, complete, 0, unroll=2)
        drain(plane_in.at[v, r], plane_sem.at[v, r % 2])
        for side, m in ((0, 0), (1, last)):
            field[v, k + 1, m] = field[v, k + 1, m] - weight * plane_in[v, r, side]
        if r == 0:
            give_back(v, 1)

        drain(edge_in.at[v, r, 1], edge_sem.at[v, r % 2, 1])
        if r in (1, 2):
            give_back(v, r + 1)
        for y in range(2):
            edge[y] = edge_in[v, r, 1, y] - weight * edge_out[v, r, 0, y]

        def outside(side, m):
            here = field[v, k, m] + jnp.concatenate(
                [
                    jnp.where(sub == 0, corner_in[v, r, 2 * side], 0.0),
                    jnp.zeros((rows - 16, lanes), jnp.float32),
                    jnp.where(sub == 7, corner_in[v, r, 2 * side + 1], 0.0),
                ],
                0,
            )
            return partial_in[v, r, side] - weight * here

        def middle(m, sums):
            return follow(v, k, m, field[v, k + 1, m - 1] + field[v, k + 1, m + 1], sums)[1]

        sums = (nothing,) * (3 if final else 5 if k == 0 else 4)
        sums = lax.fori_loop(1, last, middle, sums, unroll=2)
        drain(corner_in.at[v, r], corner_sem.at[v, r % 2])
        for y in range(2):
            for z, m in ((0, 0), (1, last)):
                edge[y, m] = edge[y, m] - weight * corner_in[v, r, 2 * z + y]
        came = partial_in.at[v, r, 1] if final else partial_in.at[v, r]
        if final:
            _, sums = follow(v, k, 0, field[v, k + 1, 1], sums)
            drain(came, partial_sem.at[v, r % 2])
            _, sums = follow(v, k, last, field[v, k + 1, last - 1] + 2.0 * outside(1, last), sums)
        else:
            drain(came, partial_sem.at[v, r % 2])
            for side, m, inner in ((0, 0, 1), (1, last, last - 1)):
                new, sums = follow(v, k, m, field[v, k + 1, inner] + outside(side, m), sums)
                put_corners(v, r + 1, side, new)
            begin(corner_copies(v, r + 1))
            begin(z_copies(v, r + 1))
            begin(y_copies(v, r + 1, 0))
            partial_faces(v, r + 1)
            partial_rest(v, r + 1)
        dots[v][2 * k + 1 : 2 * k + 4] = sums[:3]
        if not final:
            dots[v][2 * k + 4] = sums[3]
        if k == 0:
            dots[v][0] = sums[4]

    arrive(0)
    drain(level, level_sem)
    lax.fori_loop(0, GROUP, look_up, 0)
    for v in range(vecs):
        if v:
            arrive(v)
        partial_faces(v, 0)
        partial_rest(v, 0)
    for r in range(ROUNDS):
        for v in range(vecs):
            advance(v, r)

    lane = lax.broadcasted_iota(jnp.int32, (1, 128), 1)
    tile = jnp.zeros((1, 128), jnp.float32)
    for v in range(vecs):
        for d, value in enumerate(dots[v]):
            whole = jnp.sum(jnp.sum(value, axis=0, keepdims=True), axis=1, keepdims=True)
            tile = jnp.where(lane == v * len(dots[v]) + d, whole, tile)
    mine[...] = tile
    slots[me] = tile

    def tell(i, carry):
        remote(mine, slots.at[me], sum_sem.at[0], sum_sem.at[1], lax.rem(me + i, count)).start()
        return carry

    lax.fori_loop(1, count, tell, 0, unroll=8)
    others = pl.ds(0, GROUP - 1)
    drain(plane_in, sent.at[0])
    drain(field.at[:, 0, pl.ds(0, 2 * ROUNDS - 1)], sent.at[1])
    drain(edge_out, sent.at[2])
    drain(corner_out, sent.at[3])
    drain(field.at[:, 0, others], sent.at[4])
    drain(level.at[others], sent.at[5])
    drain(field.at[:, pl.ds(1, RETURNED), others], sent.at[6])
    drain(back, back_sem)
    drain(slots.at[pl.ds(0, count - 1)], sum_sem.at[0])
    drain(slots.at[pl.ds(0, count - 1)], sum_sem.at[1])
    parts = [slots[i] for i in range(count)]
    while len(parts) > 1:
        parts = [a + b for a, b in zip(parts[::2], parts[1::2])] + parts[len(parts) // 2 * 2 :]

    def spread(d):
        at = [v * 2 * LANCZOS + d for v in range(vecs)]
        return jnp.concatenate([jnp.broadcast_to(parts[0][:, i : i + 1], (1, 128)) for i in at], 0)

    nu, diag, offd = lanczos([spread(d) for d in range(2 * LANCZOS)], LANCZOS, jnp.sqrt)
    centre, width = centre[:, :128], width[:, :128]
    diag = [width * a + centre for a in diag]
    offd = [width * b for b in offd]
    third, moments = chebyshev(diag, offd, nu, centre, width)

    at = lax.broadcasted_iota(jnp.int32, small.shape[1:], 1)
    for n, items in enumerate((third, diag, offd, moments)):
        value = jnp.zeros(small.shape[1:], jnp.float32)
        for i, item in enumerate(items):
            value = jnp.where(at == i, item, value)
        small[n] = value


def finish(own, back, small, cheb, diag, offd, moments):
    vecs, lanes = own.shape[0], own.shape[2]
    for v in range(vecs):
        third = [jnp.broadcast_to(small[0, v : v + 1, k : k + 1], (1, lanes)) for k in range(RETURNED + 1)]
        value = third[0] * own[v]
        for k in range(RETURNED):
            value = value + third[k + 1] * back[k, v]
        cheb[v, 0] = value
    for n, ref in enumerate((diag, offd, moments)):
        ref[...] = small[n + 1, :, : ref.shape[1]]


def shards(count, start_vectors, levels, energies):
    vecs, _, height, lanes = start_vectors.shape
    rows = height // GROUP
    f32 = jnp.float32
    vmem = pl.BlockSpec(memory_space=pltpu.VMEM)
    dma = pltpu.SemaphoreType.DMA
    kept = pl.pallas_call(
        functools.partial(kernel, count),
        out_shape=(
            jax.ShapeDtypeStruct((vecs, height, lanes), f32),
            jax.ShapeDtypeStruct((RETURNED, vecs, height, lanes), f32),
            jax.ShapeDtypeStruct((4, vecs, 128), f32),
        ),
        in_specs=[pl.BlockSpec(memory_space=pltpu.HBM)] * 3,
        out_specs=(vmem,) * 3,
        scratch_shapes=[
            pltpu.SMEM(energies.shape, f32),
            pltpu.VMEM((height, lanes), jnp.int32),
            pltpu.VMEM((vecs, LANCZOS, GROUP, rows, lanes), f32),
            pltpu.VMEM((GROUP, rows, lanes), f32),
            pltpu.VMEM((GROUP, rows, lanes), jnp.int32),
            pltpu.VMEM((vecs, ROUNDS, 2, rows, lanes), f32),
            pltpu.VMEM((vecs, ROUNDS, 2, rows, lanes), f32),
            pltpu.VMEM((vecs, ROUNDS, 2, rows, lanes), f32),
            pltpu.VMEM((vecs, ROUNDS, 2, 2, GROUP, 1, lanes), f32),
            pltpu.VMEM((vecs, ROUNDS, 2, 2, GROUP, 1, lanes), f32),
            pltpu.VMEM((2, GROUP, 1, lanes), f32),
            pltpu.VMEM((vecs, ROUNDS, 4, 1, lanes), f32),
            pltpu.VMEM((vecs, ROUNDS, 4, 1, lanes), f32),
            pltpu.VMEM((count, 1, 128), f32),
            pltpu.VMEM((1, 128), f32),
            dma((vecs + 2,)),
            dma((vecs,)),
            dma,
            dma((vecs, 2)),
            dma((vecs, 2)),
            dma((vecs, 2, 2)),
            dma((vecs, 2)),
            dma,
            dma((2,)),
            dma((7,)),
        ],
        compiler_params=pltpu.CompilerParams(
            collective_id=0, has_side_effects=True, vmem_limit_bytes=VMEM_BYTES
        ),
    )(*(pltpu.with_memory_space_constraint(x, pltpu.HBM) for x in (energies, start_vectors, levels)))
    return pl.pallas_call(
        finish,
        out_shape=(
            jax.ShapeDtypeStruct(start_vectors.shape, f32),
            jax.ShapeDtypeStruct((vecs, LANCZOS), f32),
            jax.ShapeDtypeStruct((vecs, LANCZOS - 1), f32),
            jax.ShapeDtypeStruct((vecs, 6), f32),
        ),
        in_specs=[vmem] * 3,
        out_specs=(vmem,) * 4,
        compiler_params=pltpu.CompilerParams(vmem_limit_bytes=VMEM_BYTES),
    )(*kept)


def solution(mesh):
    in_specs = (P(None, "slab", None, None), P("slab", None, None), P())
    out_specs = (P(None, "slab", None, None), P(), P(), P())
    return jax.shard_map(
        functools.partial(shards, mesh.shape["slab"]),
        mesh=mesh, in_specs=in_specs, out_specs=out_specs, check_vma=False,
    )
```

```python
import functools

import jax
import jax.numpy as jnp
from jax import lax
from jax.experimental import pallas as pl
from jax.experimental.pallas import tpu as pltpu
from jax.sharding import PartitionSpec as P

LANCZOS = 8
ROUNDS = LANCZOS // 2
GROUP = 8
RETURNED = 3
VMEM_BYTES = 16 * 2**20


def lanczos(dots, steps, sqrt):
    inv_norm = 1.0 / dots[0]
    nu = [dots[0] * 0.0 + 1.0, dots[1] * inv_norm]
    for k in range(2, len(dots)):
        nu.append(2.0 * (dots[k] * inv_norm) - nu[k % 2])
    row, before = dict(enumerate(nu)), None
    diag, offd = [], []
    for k in range(steps):
        factor = 1.0 if k == 1 else 0.5
        alpha = row[1] if k == 0 else 0.5 * row[k + 1] - factor * before[k]
        diag.append(alpha)
        if k == steps - 1:
            break
        new = {}
        for l in range(k + 1, 2 * steps - 1 - k):
            new[l] = 0.5 * (row[l + 1] + (row[l - 1] if l - 1 > k else 1.0)) - alpha * row[l]
            if k:
                new[l] = new[l] - factor * before[l]
        first = new.pop(k + 1)
        offd.append(sqrt(first if k == 0 else 0.5 * first))
        inv = 1.0 / first
        before, row = row, {l: x * inv for l, x in new.items()}
    return nu, diag, offd


def chebyshev(diag, offd, nu, centre, width):
    left = [None] + offd
    right = offd + [None]
    low, high = None, None
    for a, b, c in zip(diag, left, right):
        reach = b if c is None else c if b is None else b + c
        low = a - reach if low is None else jnp.minimum(low, a - reach)
        high = a + reach if high is None else jnp.maximum(high, a + reach)
    inv = 1.0 / (0.55 * (high - low))
    al = width * inv
    be = (centre - 0.5 * (high + low)) * inv
    p, q, r = 2.0 * be * be + al * al - 1.0, 4.0 * al * be, al * al
    first = [be, al]
    second = [p, q, r]
    third = [2.0 * be * p + al * q - be, 2.0 * be * q + al * (2.0 * p + r) - al, 2.0 * be * r + al * q, al * r]

    def dot(f, g):
        total = None
        for i, x in enumerate(f):
            for j, y in enumerate(g):
                term = (x * y) * (0.5 * (nu[i + j] + nu[abs(i - j)]))
                total = term if total is None else total + term
        return total

    start = [nu[0]]
    m1 = dot(start, first)
    moments = [
        m1,
        dot(start, second),
        dot(start, third),
        2.0 * dot(second, second) - 1.0,
        2.0 * dot(third, second) - m1,
        2.0 * dot(third, third) - 1.0,
    ]
    return third, moments


CORES = 2


def ring_place(member):
    chip = member // CORES
    return (chip + lax.rem(chip // 2, 2) * (1 - 2 * lax.rem(chip, 2))) * CORES + lax.rem(member, CORES)


def kernel(
    count, energies, start, levels, own, back, small,
    own_energies, own_levels, field, twice, level,
    plane_in, partial_in, partial_out, edge_in, edge_out, edge, corner_in, corner_out, slots, mine,
    load_sem, vec_sem, level_sem, plane_sem, partial_sem, edge_sem, corner_sem, back_sem, sum_sem, sent,
):
    me = lax.axis_index("slab")
    member = lax.rem(me, GROUP)
    base = me - member
    vecs, _, height, lanes = start.shape
    rows = height // GROUP
    block = ring_place(member)
    mesh_id = pl.DeviceIdType.MESH
    ahead_base = lax.rem(base + GROUP, count)
    behind_base = lax.rem(base + count - GROUP, count)
    above = ring_place(lax.rem(block + GROUP - 1, GROUP))
    below = ring_place(lax.rem(block + 1, GROUP))
    last = GROUP - 1

    loads = [pltpu.make_async_copy(start.at[v, 0], own.at[v], load_sem.at[v]) for v in range(vecs)]
    loads.append(pltpu.make_async_copy(levels.at[0], own_levels, load_sem.at[vecs]))
    loads.append(pltpu.make_async_copy(energies, own_energies, load_sem.at[vecs + 1]))
    for copy in loads:
        copy.start()

    def remote(src, dst, send, recv, to):
        return pltpu.make_async_remote_copy(
            src_ref=src, dst_ref=dst, send_sem=send, recv_sem=recv, device_id=(to,), device_id_type=mesh_id
        )

    def drain(ref, sem):
        pltpu.make_async_copy(ref, ref, sem).wait()

    barrier = pltpu.get_barrier_semaphore()

    def greet(to):
        pl.semaphore_signal(barrier, inc=1, device_id=(to,), device_id_type=mesh_id)

    def greet_member(i, carry):
        greet(base + lax.rem(member + i, GROUP))
        return carry

    greet(behind_base + member)
    greet(ahead_base + member)
    lax.fori_loop(1, GROUP, greet_member, 0)
    pl.semaphore_wait(barrier, GROUP - 1 + 2)

    def rows_of(at):
        return pl.ds(pl.multiple_of(at * rows, 8), rows)

    def scatter(src, dst, send, recv):
        def body(i, carry):
            to = lax.rem(member + i, GROUP)
            remote(src.at[rows_of(ring_place(to))], dst.at[member], send, recv, base + to).start()
            return carry

        lax.fori_loop(1, GROUP, body, 0)
        pltpu.make_async_copy(src.at[rows_of(block)], dst.at[member], recv).start()

    others = pl.ds(0, GROUP - 1)
    mate = (member == 1) | (member == last - 1)

    inner = jnp.where((member == 0) | (member == last), 0, 1)

    def scatter_vec(v):
        scatter(own.at[v], field.at[v, 0], sent.at[4], vec_sem.at[v, inner])

    loads[0].wait()
    scatter_vec(0)
    loads[vecs].wait()
    scatter(own_levels, level, sent.at[5], level_sem)
    for v in range(1, vecs):
        loads[v].wait()

    @pl.when(jnp.logical_not(mate))
    def _():
        for v in range(1, vecs):
            scatter_vec(v)

    loads[vecs + 1].wait()
    values = [own_energies[i] for i in range(energies.shape[0])]
    share = 1.0 / len(values)

    def total(terms):
        return sum(terms[1:], terms[0])

    mean = total(values) * share
    apart = [x - mean for x in values]
    square = [x * x for x in apart]
    second = total(square) * share + 6.0
    cube = total([x * y for x, y in zip(square, apart)]) * share
    fourth = total([x * x for x in square]) * share + 24.0 * (second - 6.0) + 90.0
    inv_second = 1.0 / jnp.full((1, lanes), second, jnp.float32)
    skew = cube * inv_second
    centre = mean + 0.5 * skew
    width = jnp.sqrt(2.0 * (fourth * inv_second - skew * skew))
    scale = 2.0 / width

    sub = lax.broadcasted_iota(jnp.int32, (8, lanes), 0)
    zero_row = jnp.zeros((1, lanes), jnp.float32)

    def look_up(m, carry):
        ids = level[m]
        found = [jnp.full(ids.shape, x, jnp.float32) for x in values]
        bit = 1
        while len(found) > 1:
            odd = (ids & bit) != 0
            found = [
                found[i] if i + 1 == len(found) else jnp.where(odd, found[i + 1], found[i])
                for i in range(0, len(found), 2)
            ]
            bit *= 2
        twice[m] = (found[0] - centre) * scale
        return carry

    def sides():
        flip = me // (count - GROUP)
        return ((flip, jnp.where(flip == 1, ahead_base, behind_base)), (1 - flip, jnp.where(flip == 1, behind_base, ahead_base)))

    def z_copies(v, r):
        return [
            remote(
                field.at[v, 2 * r, z * last], plane_in.at[v, r, 1 - z],
                sent.at[0], plane_sem.at[v, r % 2], side + member,
            )
            for z, side in sides()
        ]

    def q_copies(v, r):
        return [
            remote(
                partial_out.at[v, r, z], partial_in.at[v, r, 1 - z],
                sent.at[1], partial_sem.at[v, r % 2], side + member,
            )
            for z, side in (((1, ahead_base),) if r == ROUNDS - 1 else sides())
        ]

    def y_copies(v, r, kind):
        return [
            remote(
                edge_out.at[v, r, kind, y], edge_in.at[v, r, kind, 1 - y],
                sent.at[2], edge_sem.at[v, r % 2, kind], base + place,
            )
            for y, place in ((0, above), (1, below))
        ]

    def corner_copies(v, r):
        return [
            remote(
                corner_out.at[v, r, 2 * z + y], corner_in.at[v, r, 2 * (1 - z) + (1 - y)],
                sent.at[3], corner_sem.at[v, r % 2], side + place,
            )
            for z, side in ((0, behind_base), (1, ahead_base))
            for y, place in ((0, above), (1, below))
        ]

    def begin(copies):
        for copy in copies:
            copy.start()

    def put_corners(v, r, z, value):
        corner_out[v, r, 2 * z] = value[0:1]
        corner_out[v, r, 2 * z + 1] = value[rows - 1 : rows]

    def put_edges(v, r, kind, m, value):
        edge_out[v, r, kind, 0, m] = value[0:1]
        edge_out[v, r, kind, 1, m] = value[rows - 1 : rows]

    def around(here, top, bottom):
        up, down = pltpu.roll(here, 1, 0), pltpu.roll(here, rows - 1, 0)
        first = jnp.where(sub == 0, top, up[0:8])
        final = jnp.where(sub == 7, bottom, down[rows - 8 :])
        near = jnp.concatenate([first, up[8:]], 0) + jnp.concatenate([down[: rows - 8], final], 0)
        return near + (pltpu.roll(here, 1, 1) + pltpu.roll(here, lanes - 1, 1))

    def partial(v, k, m, *beside):
        here = field[v, k, m]
        near = around(here, zero_row, zero_row)
        for plane in beside:
            near = near + field[v, k, plane]
        new = twice[m] * here - scale * near
        new = 0.5 * new if k == 0 else new - field[v, k - 1, m]
        field[v, k + 1, m] = new
        return new

    def tile_sum(x):
        parts = [x[i : i + 8] for i in range(0, rows, 8)]
        while len(parts) > 1:
            parts = [a + b for a, b in zip(parts[::2], parts[1::2])]
        return parts[0]

    def follow(v, k, m, near, sums):
        here, old = field[v, k + 1, m], field[v, k, m]
        near = near + around(here, edge[0, m], edge[1, m])
        new = twice[m] * here - scale * near - old
        terms = [old * here, here * here, here * new]
        if k + 2 < LANCZOS:
            field[v, k + 2, m] = new
            put_edges(v, k // 2 + 1, 0, m, new)
            terms.append(new * new)
        if k == 0:
            terms.append(old * old)
        return new, tuple(a + tile_sum(b) for a, b in zip(sums, terms))

    def give_back(v, k):
        def body(i, carry):
            to = lax.rem(member + i, GROUP)
            remote(field.at[v, k, to], back.at[k - 1, v, rows_of(block)], sent.at[6], back_sem, base + to).start()
            return carry

        lax.fori_loop(1, GROUP, body, 0)
        pltpu.make_async_copy(field.at[v, k, member], back.at[k - 1, v, rows_of(block)], back_sem).start()

    def partial_faces(v, r):
        for side, (m, inner) in enumerate(((0, 1), (last, last - 1))):
            new = partial(v, 2 * r, m, inner)
            if r < ROUNDS - 1 or side == 1:
                partial_out[v, r, side] = new
            put_edges(v, r, 1, m, new)
        begin(q_copies(v, r))

    def partial_rest(v, r):
        def body(m, carry):
            put_edges(v, r, 1, m, partial(v, 2 * r, m, m - 1, m + 1))
            return carry

        lax.fori_loop(1, last, body, 0, unroll=2)
        begin(y_copies(v, r, 1))

    def arrive(v):
        drain(field.at[v, 0, pl.ds(0, 2)], vec_sem.at[v, 0])
        for z, m in ((0, 0), (1, last)):
            corner_out[v, 0, 2 * z] = field[v, 0, m, 0:1]
            corner_out[v, 0, 2 * z + 1] = field[v, 0, m, rows - 1 : rows]
        begin(z_copies(v, 0))
        drain(field.at[v, 0, pl.ds(1, GROUP - 2)], vec_sem.at[v, 1])
        begin(corner_copies(v, 0))

        def edges(m, carry):
            edge_out[v, 0, 0, 0, m] = field[v, 0, m, 0:1]
            edge_out[v, 0, 0, 1, m] = field[v, 0, m, rows - 1 : rows]
            return carry

        lax.fori_loop(0, GROUP, edges, 0, unroll=True)
        begin(y_copies(v, 0, 0))

    nothing = jnp.zeros((8, lanes), jnp.float32)
    dots = [[None] * (2 * LANCZOS) for v in range(vecs)]

    def advance(v, r):
        k = 2 * r
        final = r == ROUNDS - 1
        weight = 0.5 * scale if k == 0 else scale

        drain(edge_in.at[v, r, 0], edge_sem.at[v, r % 2, 0])

        def complete(m, carry):
            field[v, k + 1, m, 0:8] = field[v, k + 1, m, 0:8] - jnp.where(
                sub == 0, weight * edge_in[v, r, 0, 0, m], 0.0
            )
            field[v, k + 1, m, rows - 8 : rows] = field[v, k + 1, m, rows - 8 : rows] - jnp.where(
                sub == 7, weight * edge_in[v, r, 0, 1, m], 0.0
            )
            return carry

        lax.fori_loop(0, GROUP, complete, 0, unroll=2)
        drain(plane_in.at[v, r], plane_sem.at[v, r % 2])
        for side, m in ((0, 0), (1, last)):
            field[v, k + 1, m] = field[v, k + 1, m] - weight * plane_in[v, r, side]
        if r == 0:
            give_back(v, 1)

        drain(edge_in.at[v, r, 1], edge_sem.at[v, r % 2, 1])
        if r in (1, 2):
            give_back(v, r + 1)
        for y in range(2):
            edge[y] = edge_in[v, r, 1, y] - weight * edge_out[v, r, 0, y]

        def outside(side, m):
            here = field[v, k, m] + jnp.concatenate(
                [
                    jnp.where(sub == 0, corner_in[v, r, 2 * side], 0.0),
                    jnp.zeros((rows - 16, lanes), jnp.float32),
                    jnp.where(sub == 7, corner_in[v, r, 2 * side + 1], 0.0),
                ],
                0,
            )
            return partial_in[v, r, side] - weight * here

        def middle(m, sums):
            return follow(v, k, m, field[v, k + 1, m - 1] + field[v, k + 1, m + 1], sums)[1]

        sums = (nothing,) * (3 if final else 5 if k == 0 else 4)
        sums = lax.fori_loop(1, last, middle, sums, unroll=2)
        drain(corner_in.at[v, r], corner_sem.at[v, r % 2])
        for y in range(2):
            for z, m in ((0, 0), (1, last)):
                edge[y, m] = edge[y, m] - weight * corner_in[v, r, 2 * z + y]
        came = partial_in.at[v, r, 0] if final else partial_in.at[v, r]
        if final:
            _, sums = follow(v, k, last, field[v, k + 1, last - 1], sums)
            drain(came, partial_sem.at[v, r % 2])
            _, sums = follow(v, k, 0, field[v, k + 1, 1] + 2.0 * outside(0, 0), sums)
        else:
            drain(came, partial_sem.at[v, r % 2])
            for side, m, inner in ((0, 0, 1), (1, last, last - 1)):
                new, sums = follow(v, k, m, field[v, k + 1, inner] + outside(side, m), sums)
                put_corners(v, r + 1, side, new)
            begin(corner_copies(v, r + 1))
            begin(z_copies(v, r + 1))
            begin(y_copies(v, r + 1, 0))
            partial_faces(v, r + 1)
            partial_rest(v, r + 1)
        dots[v][2 * k + 1 : 2 * k + 4] = sums[:3]
        if not final:
            dots[v][2 * k + 4] = sums[3]
        if k == 0:
            dots[v][0] = sums[4]

    arrive(0)

    @pl.when(mate)
    def _():
        drain(level.at[others], sent.at[5])
        for v in range(1, vecs):
            scatter_vec(v)

    drain(level, level_sem)
    look_up(0, 0)
    look_up(last, 0)
    for v in range(vecs):
        if v:
            arrive(v)
        partial_faces(v, 0)
        if v == 0:
            lax.fori_loop(1, last, look_up, 0)
        partial_rest(v, 0)
    for r in range(ROUNDS):
        for v in range(vecs):
            advance(v, r)

    lane = lax.broadcasted_iota(jnp.int32, (1, 128), 1)
    tile = jnp.zeros((1, 128), jnp.float32)
    for v in range(vecs):
        for d, value in enumerate(dots[v]):
            whole = jnp.sum(jnp.sum(value, axis=0, keepdims=True), axis=1, keepdims=True)
            tile = jnp.where(lane == v * len(dots[v]) + d, whole, tile)
    mine[...] = tile
    slots[me] = tile

    def tell(i, carry):
        remote(mine, slots.at[me], sum_sem.at[0], sum_sem.at[1], lax.rem(me + i, count)).start()
        return carry

    lax.fori_loop(1, count, tell, 0, unroll=8)
    drain(plane_in, sent.at[0])
    drain(field.at[:, 0, pl.ds(0, 2 * ROUNDS - 1)], sent.at[1])
    drain(edge_out, sent.at[2])
    drain(corner_out, sent.at[3])
    drain(field.at[:, 0, others], sent.at[4])

    @pl.when(jnp.logical_not(mate))
    def _():
        drain(level.at[others], sent.at[5])

    drain(field.at[:, pl.ds(1, RETURNED), others], sent.at[6])
    drain(back, back_sem)
    drain(slots.at[pl.ds(0, count - 1)], sum_sem.at[0])
    drain(slots.at[pl.ds(0, count - 1)], sum_sem.at[1])
    parts = [slots[i] for i in range(count)]
    while len(parts) > 1:
        parts = [a + b for a, b in zip(parts[::2], parts[1::2])] + parts[len(parts) // 2 * 2 :]

    def spread(d):
        at = [v * 2 * LANCZOS + d for v in range(vecs)]
        return jnp.concatenate([jnp.broadcast_to(parts[0][:, i : i + 1], (1, 128)) for i in at], 0)

    nu, diag, offd = lanczos([spread(d) for d in range(2 * LANCZOS)], LANCZOS, jnp.sqrt)
    centre, width = centre[:, :128], width[:, :128]
    diag = [width * a + centre for a in diag]
    offd = [width * b for b in offd]
    third, moments = chebyshev(diag, offd, nu, centre, width)

    at = lax.broadcasted_iota(jnp.int32, small.shape[1:], 1)
    for n, items in enumerate((third, diag, offd, moments)):
        value = jnp.zeros(small.shape[1:], jnp.float32)
        for i, item in enumerate(items):
            value = jnp.where(at == i, item, value)
        small[n] = value


def finish(own, back, small, cheb, diag, offd, moments):
    vecs, lanes = own.shape[0], own.shape[2]
    for v in range(vecs):
        third = [jnp.broadcast_to(small[0, v : v + 1, k : k + 1], (1, lanes)) for k in range(RETURNED + 1)]
        value = third[0] * own[v]
        for k in range(RETURNED):
            value = value + third[k + 1] * back[k, v]
        cheb[v, 0] = value
    for n, ref in enumerate((diag, offd, moments)):
        ref[...] = small[n + 1, :, : ref.shape[1]]


def shards(count, start_vectors, levels, energies):
    vecs, _, height, lanes = start_vectors.shape
    rows = height // GROUP
    f32 = jnp.float32
    vmem = pl.BlockSpec(memory_space=pltpu.VMEM)
    dma = pltpu.SemaphoreType.DMA
    kept = pl.pallas_call(
        functools.partial(kernel, count),
        out_shape=(
            jax.ShapeDtypeStruct((vecs, height, lanes), f32),
            jax.ShapeDtypeStruct((RETURNED, vecs, height, lanes), f32),
            jax.ShapeDtypeStruct((4, vecs, 128), f32),
        ),
        in_specs=[pl.BlockSpec(memory_space=pltpu.HBM)] * 3,
        out_specs=(vmem,) * 3,
        scratch_shapes=[
            pltpu.SMEM(energies.shape, f32),
            pltpu.VMEM((height, lanes), jnp.int32),
            pltpu.VMEM((vecs, LANCZOS, GROUP, rows, lanes), f32),
            pltpu.VMEM((GROUP, rows, lanes), f32),
            pltpu.VMEM((GROUP, rows, lanes), jnp.int32),
            pltpu.VMEM((vecs, ROUNDS, 2, rows, lanes), f32),
            pltpu.VMEM((vecs, ROUNDS, 2, rows, lanes), f32),
            pltpu.VMEM((vecs, ROUNDS, 2, rows, lanes), f32),
            pltpu.VMEM((vecs, ROUNDS, 2, 2, GROUP, 1, lanes), f32),
            pltpu.VMEM((vecs, ROUNDS, 2, 2, GROUP, 1, lanes), f32),
            pltpu.VMEM((2, GROUP, 1, lanes), f32),
            pltpu.VMEM((vecs, ROUNDS, 4, 1, lanes), f32),
            pltpu.VMEM((vecs, ROUNDS, 4, 1, lanes), f32),
            pltpu.VMEM((count, 1, 128), f32),
            pltpu.VMEM((1, 128), f32),
            dma((vecs + 2,)),
            dma((vecs, 2)),
            dma,
            dma((vecs, 2)),
            dma((vecs, 2)),
            dma((vecs, 2, 2)),
            dma((vecs, 2)),
            dma,
            dma((2,)),
            dma((7,)),
        ],
        compiler_params=pltpu.CompilerParams(
            collective_id=0, has_side_effects=True, vmem_limit_bytes=VMEM_BYTES
        ),
    )(*(pltpu.with_memory_space_constraint(x, pltpu.HBM) for x in (energies, start_vectors, levels)))
    return pl.pallas_call(
        finish,
        out_shape=(
            jax.ShapeDtypeStruct(start_vectors.shape, f32),
            jax.ShapeDtypeStruct((vecs, LANCZOS), f32),
            jax.ShapeDtypeStruct((vecs, LANCZOS - 1), f32),
            jax.ShapeDtypeStruct((vecs, 6), f32),
        ),
        in_specs=[vmem] * 3,
        out_specs=(vmem,) * 4,
        compiler_params=pltpu.CompilerParams(vmem_limit_bytes=VMEM_BYTES),
    )(*kept)


def solution(mesh):
    in_specs = (P(None, "slab", None, None), P("slab", None, None), P())
    out_specs = (P(None, "slab", None, None), P(), P(), P())
    return jax.shard_map(
        functools.partial(shards, mesh.shape["slab"]),
        mesh=mesh, in_specs=in_specs, out_specs=out_specs, check_vma=False,
    )
```

```python
import functools

import jax
import jax.numpy as jnp
from jax import lax
from jax.experimental import pallas as pl
from jax.experimental.pallas import tpu as pltpu
from jax.sharding import PartitionSpec as P

LANCZOS = 8
ROUNDS = LANCZOS // 2
GROUP = 8
RETURNED = 3
VMEM_BYTES = 16 * 2**20


def lanczos(dots, steps, sqrt):
    inv_norm = 1.0 / dots[0]
    nu = [dots[0] * 0.0 + 1.0, dots[1] * inv_norm]
    for k in range(2, len(dots)):
        nu.append(2.0 * (dots[k] * inv_norm) - nu[k % 2])
    row, before = dict(enumerate(nu)), None
    diag, offd = [], []
    for k in range(steps):
        factor = 1.0 if k == 1 else 0.5
        alpha = row[1] if k == 0 else 0.5 * row[k + 1] - factor * before[k]
        diag.append(alpha)
        if k == steps - 1:
            break
        new = {}
        for l in range(k + 1, 2 * steps - 1 - k):
            new[l] = 0.5 * (row[l + 1] + (row[l - 1] if l - 1 > k else 1.0)) - alpha * row[l]
            if k:
                new[l] = new[l] - factor * before[l]
        first = new.pop(k + 1)
        offd.append(sqrt(first if k == 0 else 0.5 * first))
        inv = 1.0 / first
        before, row = row, {l: x * inv for l, x in new.items()}
    return nu, diag, offd


def chebyshev(diag, offd, nu, centre, width):
    left = [None] + offd
    right = offd + [None]
    low, high = None, None
    for a, b, c in zip(diag, left, right):
        reach = b if c is None else c if b is None else b + c
        low = a - reach if low is None else jnp.minimum(low, a - reach)
        high = a + reach if high is None else jnp.maximum(high, a + reach)
    inv = 1.0 / (0.55 * (high - low))
    al = width * inv
    be = (centre - 0.5 * (high + low)) * inv
    p, q, r = 2.0 * be * be + al * al - 1.0, 4.0 * al * be, al * al
    first = [be, al]
    second = [p, q, r]
    third = [2.0 * be * p + al * q - be, 2.0 * be * q + al * (2.0 * p + r) - al, 2.0 * be * r + al * q, al * r]

    def dot(f, g):
        total = None
        for i, x in enumerate(f):
            for j, y in enumerate(g):
                term = (x * y) * (0.5 * (nu[i + j] + nu[abs(i - j)]))
                total = term if total is None else total + term
        return total

    start = [nu[0]]
    m1 = dot(start, first)
    moments = [
        m1,
        dot(start, second),
        dot(start, third),
        2.0 * dot(second, second) - 1.0,
        2.0 * dot(third, second) - m1,
        2.0 * dot(third, third) - 1.0,
    ]
    return third, moments


CORES = 2


def ring_place(member):
    chip = member // CORES
    return (chip + lax.rem(chip // 2, 2) * (1 - 2 * lax.rem(chip, 2))) * CORES + lax.rem(member, CORES)


def kernel(
    count, energies, start, levels, own, back, small,
    own_energies, own_levels, field, twice, level,
    plane_in, partial_in, partial_out, edge_in, edge_out, edge, corner_in, corner_out, slots, mine,
    load_sem, vec_sem, level_sem, plane_sem, partial_sem, edge_sem, corner_sem, back_sem, sum_sem, sent,
):
    me = lax.axis_index("slab")
    member = lax.rem(me, GROUP)
    base = me - member
    vecs, _, height, lanes = start.shape
    rows = height // GROUP
    block = ring_place(member)
    mesh_id = pl.DeviceIdType.MESH
    ahead_base = lax.rem(base + GROUP, count)
    behind_base = lax.rem(base + count - GROUP, count)
    above = ring_place(lax.rem(block + GROUP - 1, GROUP))
    below = ring_place(lax.rem(block + 1, GROUP))
    last = GROUP - 1

    loads = [pltpu.make_async_copy(start.at[v, 0], own.at[v], load_sem.at[v]) for v in range(vecs)]
    loads.append(pltpu.make_async_copy(levels.at[0], own_levels, load_sem.at[vecs]))
    loads.append(pltpu.make_async_copy(energies, own_energies, load_sem.at[vecs + 1]))
    for copy in loads:
        copy.start()

    def remote(src, dst, send, recv, to):
        return pltpu.make_async_remote_copy(
            src_ref=src, dst_ref=dst, send_sem=send, recv_sem=recv, device_id=(to,), device_id_type=mesh_id
        )

    def drain(ref, sem):
        pltpu.make_async_copy(ref, ref, sem).wait()

    barrier = pltpu.get_barrier_semaphore()

    def greet(to):
        pl.semaphore_signal(barrier, inc=1, device_id=(to,), device_id_type=mesh_id)

    def greet_member(i, carry):
        greet(base + lax.rem(member + i, GROUP))
        return carry

    greet(behind_base + member)
    greet(ahead_base + member)
    lax.fori_loop(1, GROUP, greet_member, 0)
    pl.semaphore_wait(barrier, GROUP - 1 + 2)

    def rows_of(at):
        return pl.ds(pl.multiple_of(at * rows, 8), rows)

    def scatter(src, dst, send, recv):
        def body(i, carry):
            to = lax.rem(member + i, GROUP)
            remote(src.at[rows_of(ring_place(to))], dst.at[member], send, recv, base + to).start()
            return carry

        lax.fori_loop(1, GROUP, body, 0)
        pltpu.make_async_copy(src.at[rows_of(block)], dst.at[member], recv).start()

    others = pl.ds(0, GROUP - 1)
    mate = (member == 1) | (member == last - 1)

    inner = jnp.where((member == 0) | (member == last), 0, 1)

    def scatter_vec(v):
        scatter(own.at[v], field.at[v, 0], sent.at[4], vec_sem.at[v, inner])

    loads[0].wait()
    scatter_vec(0)
    loads[vecs].wait()
    scatter(own_levels, level, sent.at[5], level_sem)
    for v in range(1, vecs):
        loads[v].wait()

    @pl.when(jnp.logical_not(mate))
    def _():
        for v in range(1, vecs):
            scatter_vec(v)

    loads[vecs + 1].wait()
    values = [own_energies[i] for i in range(energies.shape[0])]
    share = 1.0 / len(values)

    def total(terms):
        return sum(terms[1:], terms[0])

    mean = total(values) * share
    apart = [x - mean for x in values]
    square = [x * x for x in apart]
    second = total(square) * share + 6.0
    cube = total([x * y for x, y in zip(square, apart)]) * share
    fourth = total([x * x for x in square]) * share + 24.0 * (second - 6.0) + 90.0
    inv_second = 1.0 / jnp.full((1, lanes), second, jnp.float32)
    skew = cube * inv_second
    centre = mean + 0.5 * skew
    width = jnp.sqrt(2.0 * (fourth * inv_second - skew * skew))
    scale = 2.0 / width

    sub = lax.broadcasted_iota(jnp.int32, (8, lanes), 0)
    zero_row = jnp.zeros((1, lanes), jnp.float32)

    def look_up(m, carry):
        ids = level[m]
        found = [jnp.full(ids.shape, x, jnp.float32) for x in values]
        bit = 1
        while len(found) > 1:
            odd = (ids & bit) != 0
            found = [
                found[i] if i + 1 == len(found) else jnp.where(odd, found[i + 1], found[i])
                for i in range(0, len(found), 2)
            ]
            bit *= 2
        twice[m] = (found[0] - centre) * scale
        return carry

    def sides():
        flip = me // (count - GROUP)
        return ((flip, jnp.where(flip == 1, ahead_base, behind_base)), (1 - flip, jnp.where(flip == 1, behind_base, ahead_base)))

    def z_copies(v, r):
        return [
            remote(
                field.at[v, 2 * r, z * last], plane_in.at[v, r, 1 - z],
                sent.at[0], plane_sem.at[v, r % 2], side + member,
            )
            for z, side in sides()
        ]

    def q_copies(v, r):
        return [
            remote(
                partial_out.at[v, r, z], partial_in.at[v, r, 1 - z],
                sent.at[1], partial_sem.at[v, r % 2], side + member,
            )
            for z, side in (((1, ahead_base),) if r == ROUNDS - 1 else sides())
        ]

    def y_copies(v, r):
        return [
            remote(
                edge_out.at[v, r, y], edge_in.at[v, r, 1 - y],
                sent.at[2], edge_sem.at[v, r % 2], base + place,
            )
            for y, place in ((0, above), (1, below))
        ]

    def corner_copies(v, r):
        return [
            remote(
                corner_out.at[v, r, 2 * z + y], corner_in.at[v, r, 2 * (1 - z) + (1 - y)],
                sent.at[3], corner_sem.at[v, r % 2], side + place,
            )
            for z, side in ((0, behind_base), (1, ahead_base))
            for y, place in ((0, above), (1, below))
        ]

    def begin(copies):
        for copy in copies:
            copy.start()

    def put_corners(v, r, z, value):
        corner_out[v, r, 2 * z] = value[0:1]
        corner_out[v, r, 2 * z + 1] = value[rows - 1 : rows]

    def put_edges(v, r, kind, m, value):
        edge_out[v, r, 0, kind, m] = value[0:1]
        edge_out[v, r, 1, kind, m] = value[rows - 1 : rows]

    def around(here, top, bottom):
        up, down = pltpu.roll(here, 1, 0), pltpu.roll(here, rows - 1, 0)
        first = jnp.where(sub == 0, top, up[0:8])
        final = jnp.where(sub == 7, bottom, down[rows - 8 :])
        near = jnp.concatenate([first, up[8:]], 0) + jnp.concatenate([down[: rows - 8], final], 0)
        return near + (pltpu.roll(here, 1, 1) + pltpu.roll(here, lanes - 1, 1))

    def partial(v, k, m, *beside):
        here = field[v, k, m]
        near = around(here, zero_row, zero_row)
        for plane in beside:
            near = near + field[v, k, plane]
        new = twice[m] * here - scale * near
        new = 0.5 * new if k == 0 else new - field[v, k - 1, m]
        field[v, k + 1, m] = new
        return new

    def tile_sum(x):
        parts = [x[i : i + 8] for i in range(0, rows, 8)]
        while len(parts) > 1:
            parts = [a + b for a, b in zip(parts[::2], parts[1::2])]
        return parts[0]

    def follow(v, k, m, near, sums):
        here, old = field[v, k + 1, m], field[v, k, m]
        near = near + around(here, edge[0, m], edge[1, m])
        new = twice[m] * here - scale * near - old
        terms = [old * here, here * here, here * new]
        if k + 2 < LANCZOS:
            field[v, k + 2, m] = new
            put_edges(v, k // 2 + 1, 0, m, new)
            terms.append(new * new)
        if k == 0:
            terms.append(old * old)
        return new, tuple(a + tile_sum(b) for a, b in zip(sums, terms))

    def give_back(v, k):
        def body(i, carry):
            to = lax.rem(member + i, GROUP)
            remote(field.at[v, k, to], back.at[k - 1, v, rows_of(block)], sent.at[6], back_sem, base + to).start()
            return carry

        lax.fori_loop(1, GROUP, body, 0)
        pltpu.make_async_copy(field.at[v, k, member], back.at[k - 1, v, rows_of(block)], back_sem).start()

    def partial_faces(v, r):
        for side, (m, inner) in enumerate(((0, 1), (last, last - 1))):
            new = partial(v, 2 * r, m, inner)
            if r < ROUNDS - 1 or side == 1:
                partial_out[v, r, side] = new
            put_edges(v, r, 1, m, new)
        begin(q_copies(v, r))

    def partial_rest(v, r):
        def body(m, carry):
            put_edges(v, r, 1, m, partial(v, 2 * r, m, m - 1, m + 1))
            return carry

        lax.fori_loop(1, last, body, 0, unroll=2)
        begin(y_copies(v, r))

    def arrive(v):
        drain(field.at[v, 0, pl.ds(0, 2)], vec_sem.at[v, 0])
        for z, m in ((0, 0), (1, last)):
            corner_out[v, 0, 2 * z] = field[v, 0, m, 0:1]
            corner_out[v, 0, 2 * z + 1] = field[v, 0, m, rows - 1 : rows]
        begin(z_copies(v, 0))
        drain(field.at[v, 0, pl.ds(1, GROUP - 2)], vec_sem.at[v, 1])
        begin(corner_copies(v, 0))

        def edges(m, carry):
            edge_out[v, 0, 0, 0, m] = field[v, 0, m, 0:1]
            edge_out[v, 0, 1, 0, m] = field[v, 0, m, rows - 1 : rows]
            return carry

        lax.fori_loop(0, GROUP, edges, 0, unroll=True)

    nothing = jnp.zeros((8, lanes), jnp.float32)
    dots = [[None] * (2 * LANCZOS) for v in range(vecs)]

    def advance(v, r):
        k = 2 * r
        final = r == ROUNDS - 1
        weight = 0.5 * scale if k == 0 else scale

        drain(edge_in.at[v, r], edge_sem.at[v, r % 2])

        def complete(m, carry):
            field[v, k + 1, m, 0:8] = field[v, k + 1, m, 0:8] - jnp.where(
                sub == 0, weight * edge_in[v, r, 0, 0, m], 0.0
            )
            field[v, k + 1, m, rows - 8 : rows] = field[v, k + 1, m, rows - 8 : rows] - jnp.where(
                sub == 7, weight * edge_in[v, r, 1, 0, m], 0.0
            )
            return carry

        lax.fori_loop(0, GROUP, complete, 0, unroll=2)
        drain(plane_in.at[v, r], plane_sem.at[v, r % 2])
        for side, m in ((0, 0), (1, last)):
            field[v, k + 1, m] = field[v, k + 1, m] - weight * plane_in[v, r, side]
        if r == 0:
            give_back(v, 1)

        if r in (1, 2):
            give_back(v, r + 1)
        for y in range(2):
            edge[y] = edge_in[v, r, y, 1] - weight * edge_out[v, r, y, 0]

        def outside(side, m):
            here = field[v, k, m] + jnp.concatenate(
                [
                    jnp.where(sub == 0, corner_in[v, r, 2 * side], 0.0),
                    jnp.zeros((rows - 16, lanes), jnp.float32),
                    jnp.where(sub == 7, corner_in[v, r, 2 * side + 1], 0.0),
                ],
                0,
            )
            return partial_in[v, r, side] - weight * here

        def middle(m, sums):
            return follow(v, k, m, field[v, k + 1, m - 1] + field[v, k + 1, m + 1], sums)[1]

        sums = (nothing,) * (3 if final else 5 if k == 0 else 4)
        sums = lax.fori_loop(1, last, middle, sums, unroll=2)
        drain(corner_in.at[v, r], corner_sem.at[v, r % 2])
        for y in range(2):
            for z, m in ((0, 0), (1, last)):
                edge[y, m] = edge[y, m] - weight * corner_in[v, r, 2 * z + y]
        came = partial_in.at[v, r, 0] if final else partial_in.at[v, r]
        if final:
            _, sums = follow(v, k, last, field[v, k + 1, last - 1], sums)
            drain(came, partial_sem.at[v, r % 2])
            _, sums = follow(v, k, 0, field[v, k + 1, 1] + 2.0 * outside(0, 0), sums)
        else:
            drain(came, partial_sem.at[v, r % 2])
            for side, m, inner in ((0, 0, 1), (1, last, last - 1)):
                new, sums = follow(v, k, m, field[v, k + 1, inner] + outside(side, m), sums)
                put_corners(v, r + 1, side, new)
            begin(corner_copies(v, r + 1))
            begin(z_copies(v, r + 1))
            partial_faces(v, r + 1)
            partial_rest(v, r + 1)
        dots[v][2 * k + 1 : 2 * k + 4] = sums[:3]
        if not final:
            dots[v][2 * k + 4] = sums[3]
        if k == 0:
            dots[v][0] = sums[4]

    arrive(0)

    @pl.when(mate)
    def _():
        drain(level.at[others], sent.at[5])
        for v in range(1, vecs):
            scatter_vec(v)

    drain(level, level_sem)
    look_up(0, 0)
    look_up(last, 0)
    for v in range(vecs):
        if v:
            arrive(v)
        partial_faces(v, 0)
        if v == 0:
            lax.fori_loop(1, last, look_up, 0)
        partial_rest(v, 0)
    for r in range(ROUNDS):
        for v in range(vecs):
            advance(v, r)

    lane = lax.broadcasted_iota(jnp.int32, (1, 128), 1)
    tile = jnp.zeros((1, 128), jnp.float32)
    for v in range(vecs):
        for d, value in enumerate(dots[v]):
            whole = jnp.sum(jnp.sum(value, axis=0, keepdims=True), axis=1, keepdims=True)
            tile = jnp.where(lane == v * len(dots[v]) + d, whole, tile)
    mine[...] = tile
    slots[me] = tile

    def tell(i, carry):
        remote(mine, slots.at[me], sum_sem.at[0], sum_sem.at[1], lax.rem(me + i, count)).start()
        return carry

    lax.fori_loop(1, count, tell, 0, unroll=8)
    drain(plane_in, sent.at[0])
    drain(field.at[:, 0, pl.ds(0, 2 * ROUNDS - 1)], sent.at[1])
    drain(edge_out, sent.at[2])
    drain(corner_out, sent.at[3])
    drain(field.at[:, 0, others], sent.at[4])

    @pl.when(jnp.logical_not(mate))
    def _():
        drain(level.at[others], sent.at[5])

    drain(field.at[:, pl.ds(1, RETURNED), others], sent.at[6])
    drain(back, back_sem)
    drain(slots.at[pl.ds(0, count - 1)], sum_sem.at[0])
    drain(slots.at[pl.ds(0, count - 1)], sum_sem.at[1])
    parts = [slots[i] for i in range(count)]
    while len(parts) > 1:
        parts = [a + b for a, b in zip(parts[::2], parts[1::2])] + parts[len(parts) // 2 * 2 :]

    def spread(d):
        at = [v * 2 * LANCZOS + d for v in range(vecs)]
        return jnp.concatenate([jnp.broadcast_to(parts[0][:, i : i + 1], (1, 128)) for i in at], 0)

    nu, diag, offd = lanczos([spread(d) for d in range(2 * LANCZOS)], LANCZOS, jnp.sqrt)
    centre, width = centre[:, :128], width[:, :128]
    diag = [width * a + centre for a in diag]
    offd = [width * b for b in offd]
    third, moments = chebyshev(diag, offd, nu, centre, width)

    at = lax.broadcasted_iota(jnp.int32, small.shape[1:], 1)
    for n, items in enumerate((third, diag, offd, moments)):
        value = jnp.zeros(small.shape[1:], jnp.float32)
        for i, item in enumerate(items):
            value = jnp.where(at == i, item, value)
        small[n] = value


def finish(own, back, small, cheb, diag, offd, moments):
    vecs, lanes = own.shape[0], own.shape[2]
    for v in range(vecs):
        third = [jnp.broadcast_to(small[0, v : v + 1, k : k + 1], (1, lanes)) for k in range(RETURNED + 1)]
        value = third[0] * own[v]
        for k in range(RETURNED):
            value = value + third[k + 1] * back[k, v]
        cheb[v, 0] = value
    for n, ref in enumerate((diag, offd, moments)):
        ref[...] = small[n + 1, :, : ref.shape[1]]


def shards(count, start_vectors, levels, energies):
    vecs, _, height, lanes = start_vectors.shape
    rows = height // GROUP
    f32 = jnp.float32
    vmem = pl.BlockSpec(memory_space=pltpu.VMEM)
    dma = pltpu.SemaphoreType.DMA
    kept = pl.pallas_call(
        functools.partial(kernel, count),
        out_shape=(
            jax.ShapeDtypeStruct((vecs, height, lanes), f32),
            jax.ShapeDtypeStruct((RETURNED, vecs, height, lanes), f32),
            jax.ShapeDtypeStruct((4, vecs, 128), f32),
        ),
        in_specs=[pl.BlockSpec(memory_space=pltpu.HBM)] * 3,
        out_specs=(vmem,) * 3,
        scratch_shapes=[
            pltpu.SMEM(energies.shape, f32),
            pltpu.VMEM((height, lanes), jnp.int32),
            pltpu.VMEM((vecs, LANCZOS, GROUP, rows, lanes), f32),
            pltpu.VMEM((GROUP, rows, lanes), f32),
            pltpu.VMEM((GROUP, rows, lanes), jnp.int32),
            pltpu.VMEM((vecs, ROUNDS, 2, rows, lanes), f32),
            pltpu.VMEM((vecs, ROUNDS, 2, rows, lanes), f32),
            pltpu.VMEM((vecs, ROUNDS, 2, rows, lanes), f32),
            pltpu.VMEM((vecs, ROUNDS, 2, 2, GROUP, 1, lanes), f32),
            pltpu.VMEM((vecs, ROUNDS, 2, 2, GROUP, 1, lanes), f32),
            pltpu.VMEM((2, GROUP, 1, lanes), f32),
            pltpu.VMEM((vecs, ROUNDS, 4, 1, lanes), f32),
            pltpu.VMEM((vecs, ROUNDS, 4, 1, lanes), f32),
            pltpu.VMEM((count, 1, 128), f32),
            pltpu.VMEM((1, 128), f32),
            dma((vecs + 2,)),
            dma((vecs, 2)),
            dma,
            dma((vecs, 2)),
            dma((vecs, 2)),
            dma((vecs, 2)),
            dma((vecs, 2)),
            dma,
            dma((2,)),
            dma((7,)),
        ],
        compiler_params=pltpu.CompilerParams(
            collective_id=0, has_side_effects=True, vmem_limit_bytes=VMEM_BYTES
        ),
    )(*(pltpu.with_memory_space_constraint(x, pltpu.HBM) for x in (energies, start_vectors, levels)))
    return pl.pallas_call(
        finish,
        out_shape=(
            jax.ShapeDtypeStruct(start_vectors.shape, f32),
            jax.ShapeDtypeStruct((vecs, LANCZOS), f32),
            jax.ShapeDtypeStruct((vecs, LANCZOS - 1), f32),
            jax.ShapeDtypeStruct((vecs, 6), f32),
        ),
        in_specs=[vmem] * 3,
        out_specs=(vmem,) * 4,
        compiler_params=pltpu.CompilerParams(vmem_limit_bytes=VMEM_BYTES),
    )(*kept)


def solution(mesh):
    in_specs = (P(None, "slab", None, None), P("slab", None, None), P())
    out_specs = (P(None, "slab", None, None), P(), P(), P())
    return jax.shard_map(
        functools.partial(shards, mesh.shape["slab"]),
        mesh=mesh, in_specs=in_specs, out_specs=out_specs, check_vma=False,
    )
```

```python
import functools

import jax
import jax.numpy as jnp
from jax import lax
from jax.experimental import pallas as pl
from jax.experimental.pallas import tpu as pltpu
from jax.sharding import PartitionSpec as P

LANCZOS = 8
ROUNDS = LANCZOS // 2
GROUP = 8
RETURNED = 3
VMEM_BYTES = 16 * 2**20


def lanczos(dots, steps, sqrt):
    inv_norm = 1.0 / dots[0]
    nu = [dots[0] * 0.0 + 1.0, dots[1] * inv_norm]
    for k in range(2, len(dots)):
        nu.append(2.0 * (dots[k] * inv_norm) - nu[k % 2])
    row, before = dict(enumerate(nu)), None
    diag, offd = [], []
    for k in range(steps):
        factor = 1.0 if k == 1 else 0.5
        alpha = row[1] if k == 0 else 0.5 * row[k + 1] - factor * before[k]
        diag.append(alpha)
        if k == steps - 1:
            break
        new = {}
        for l in range(k + 1, 2 * steps - 1 - k):
            new[l] = 0.5 * (row[l + 1] + (row[l - 1] if l - 1 > k else 1.0)) - alpha * row[l]
            if k:
                new[l] = new[l] - factor * before[l]
        first = new.pop(k + 1)
        offd.append(sqrt(first if k == 0 else 0.5 * first))
        inv = 1.0 / first
        before, row = row, {l: x * inv for l, x in new.items()}
    return nu, diag, offd


def chebyshev(diag, offd, nu, centre, width):
    left = [None] + offd
    right = offd + [None]
    low, high = None, None
    for a, b, c in zip(diag, left, right):
        reach = b if c is None else c if b is None else b + c
        low = a - reach if low is None else jnp.minimum(low, a - reach)
        high = a + reach if high is None else jnp.maximum(high, a + reach)
    inv = 1.0 / (0.55 * (high - low))
    al = width * inv
    be = (centre - 0.5 * (high + low)) * inv
    p, q, r = 2.0 * be * be + al * al - 1.0, 4.0 * al * be, al * al
    first = [be, al]
    second = [p, q, r]
    third = [2.0 * be * p + al * q - be, 2.0 * be * q + al * (2.0 * p + r) - al, 2.0 * be * r + al * q, al * r]

    def dot(f, g):
        total = None
        for i, x in enumerate(f):
            for j, y in enumerate(g):
                term = (x * y) * (0.5 * (nu[i + j] + nu[abs(i - j)]))
                total = term if total is None else total + term
        return total

    start = [nu[0]]
    m1 = dot(start, first)
    moments = [
        m1,
        dot(start, second),
        dot(start, third),
        2.0 * dot(second, second) - 1.0,
        2.0 * dot(third, second) - m1,
        2.0 * dot(third, third) - 1.0,
    ]
    return third, moments


CORES = 2


def ring_place(member):
    chip = member // CORES
    return (chip + lax.rem(chip // 2, 2) * (1 - 2 * lax.rem(chip, 2))) * CORES + lax.rem(member, CORES)


def kernel(
    count, energies, start, levels, own, back, small,
    own_energies, own_levels, field, twice, level,
    plane_in, partial_in, partial_out, edge_in, edge_out, edge, corner_in, corner_out, slots, mine,
    load_sem, vec_sem, level_sem, plane_sem, partial_sem, edge_sem, corner_sem, back_sem, sum_sem, sent,
):
    me = lax.axis_index("slab")
    member = lax.rem(me, GROUP)
    base = me - member
    vecs, _, height, lanes = start.shape
    rows = height // GROUP
    block = ring_place(member)
    mesh_id = pl.DeviceIdType.MESH
    ahead_base = lax.rem(base + GROUP, count)
    behind_base = lax.rem(base + count - GROUP, count)
    above = ring_place(lax.rem(block + GROUP - 1, GROUP))
    below = ring_place(lax.rem(block + 1, GROUP))
    last = GROUP - 1

    loads = [pltpu.make_async_copy(start.at[v, 0], own.at[v], load_sem.at[v]) for v in range(vecs)]
    loads.append(pltpu.make_async_copy(levels.at[0], own_levels, load_sem.at[vecs]))
    loads.append(pltpu.make_async_copy(energies, own_energies, load_sem.at[vecs + 1]))
    for copy in loads:
        copy.start()

    def remote(src, dst, send, recv, to):
        return pltpu.make_async_remote_copy(
            src_ref=src, dst_ref=dst, send_sem=send, recv_sem=recv, device_id=(to,), device_id_type=mesh_id
        )

    def drain(ref, sem):
        pltpu.make_async_copy(ref, ref, sem).wait()

    barrier = pltpu.get_barrier_semaphore()

    def greet(to):
        pl.semaphore_signal(barrier, inc=1, device_id=(to,), device_id_type=mesh_id)

    def greet_member(i, carry):
        greet(base + lax.rem(member + i, GROUP))
        return carry

    greet(behind_base + member)
    greet(ahead_base + member)
    lax.fori_loop(1, GROUP, greet_member, 0)
    pl.semaphore_wait(barrier, GROUP - 1 + 2)

    def rows_of(at):
        return pl.ds(pl.multiple_of(at * rows, 8), rows)

    def scatter(src, dst, send, recv):
        def body(i, carry):
            to = lax.rem(member + i, GROUP)
            remote(src.at[rows_of(ring_place(to))], dst.at[member], send, recv, base + to).start()
            return carry

        lax.fori_loop(1, GROUP, body, 0)
        pltpu.make_async_copy(src.at[rows_of(block)], dst.at[member], recv).start()

    others = pl.ds(0, GROUP - 1)
    mate = (member == 1) | (member == last - 1)

    inner = jnp.where((member == 0) | (member == last), 0, 1)

    def scatter_vec(v):
        scatter(own.at[v], field.at[v, 0], sent.at[4], vec_sem.at[v, inner])

    loads[0].wait()
    scatter_vec(0)
    loads[vecs].wait()
    scatter(own_levels, level, sent.at[5], level_sem)
    for v in range(1, vecs):
        loads[v].wait()

    @pl.when(jnp.logical_not(mate))
    def _():
        for v in range(1, vecs):
            scatter_vec(v)

    loads[vecs + 1].wait()
    values = [own_energies[i] for i in range(energies.shape[0])]
    share = 1.0 / len(values)

    def total(terms):
        return sum(terms[1:], terms[0])

    mean = total(values) * share
    apart = [x - mean for x in values]
    square = [x * x for x in apart]
    second = total(square) * share + 6.0
    cube = total([x * y for x, y in zip(square, apart)]) * share
    fourth = total([x * x for x in square]) * share + 24.0 * (second - 6.0) + 90.0
    inv_second = 1.0 / jnp.full((1, lanes), second, jnp.float32)
    skew = cube * inv_second
    centre = mean + 0.5 * skew
    width = jnp.sqrt(2.0 * (fourth * inv_second - skew * skew))
    scale = 2.0 / width

    sub = lax.broadcasted_iota(jnp.int32, (8, lanes), 0)
    zero_row = jnp.zeros((1, lanes), jnp.float32)

    def look_up(m, carry):
        ids = level[m]
        found = [jnp.full(ids.shape, x, jnp.float32) for x in values]
        bit = 1
        while len(found) > 1:
            odd = (ids & bit) != 0
            found = [
                found[i] if i + 1 == len(found) else jnp.where(odd, found[i + 1], found[i])
                for i in range(0, len(found), 2)
            ]
            bit *= 2
        twice[m] = (found[0] - centre) * scale
        return carry

    def sides():
        flip = me // (count - GROUP)
        return ((flip, jnp.where(flip == 1, ahead_base, behind_base)), (1 - flip, jnp.where(flip == 1, behind_base, ahead_base)))

    def z_copies(v, r):
        return [
            remote(
                field.at[v, 2 * r, z * last], plane_in.at[v, r, 1 - z],
                sent.at[0], plane_sem.at[v, r % 2], side + member,
            )
            for z, side in sides()
        ]

    def q_copies(v, r):
        return [
            remote(
                partial_out.at[v, r, z], partial_in.at[v, r, 1 - z],
                sent.at[1], partial_sem.at[v, r % 2], side + member,
            )
            for z, side in (((1, ahead_base),) if r == ROUNDS - 1 else sides())
        ]

    def y_copies(v, r):
        return [
            remote(
                edge_out.at[v, r, y], edge_in.at[v, r, 1 - y],
                sent.at[2], edge_sem.at[v, r % 2], base + place,
            )
            for y, place in ((0, above), (1, below))
        ]

    def corner_copies(v, r):
        return [
            remote(
                corner_out.at[v, r, 2 * z + y], corner_in.at[v, r, 2 * (1 - z) + (1 - y)],
                sent.at[3], corner_sem.at[v, r % 2], side + place,
            )
            for z, side in ((0, behind_base), (1, ahead_base))
            for y, place in ((0, above), (1, below))
        ]

    def begin(copies):
        for copy in copies:
            copy.start()

    def put_corners(v, r, z, value):
        corner_out[v, r, 2 * z] = value[0:1]
        corner_out[v, r, 2 * z + 1] = value[rows - 1 : rows]

    def put_edges(v, r, kind, m, value):
        edge_out[v, r, 0, kind, m] = value[0:1]
        edge_out[v, r, 1, kind, m] = value[rows - 1 : rows]

    def around(here, top, bottom):
        up, down = pltpu.roll(here, 1, 0), pltpu.roll(here, rows - 1, 0)
        first = jnp.where(sub == 0, top, up[0:8])
        final = jnp.where(sub == 7, bottom, down[rows - 8 :])
        near = jnp.concatenate([first, up[8:]], 0) + jnp.concatenate([down[: rows - 8], final], 0)
        return near + (pltpu.roll(here, 1, 1) + pltpu.roll(here, lanes - 1, 1))

    def partial(v, k, m, *beside):
        here = field[v, k, m]
        near = around(here, zero_row, zero_row)
        for plane in beside:
            near = near + field[v, k, plane]
        new = twice[m] * here - scale * near
        new = 0.5 * new if k == 0 else new - field[v, k - 1, m]
        field[v, k + 1, m] = new
        return new

    def tile_sum(x):
        parts = [x[i : i + 8] for i in range(0, rows, 8)]
        while len(parts) > 1:
            parts = [a + b for a, b in zip(parts[::2], parts[1::2])]
        return parts[0]

    def follow(v, k, m, near, sums):
        here, old = field[v, k + 1, m], field[v, k, m]
        near = near + around(here, edge[0, m], edge[1, m])
        new = twice[m] * here - scale * near - old
        terms = [old * here, here * here, here * new]
        if k + 2 < LANCZOS:
            field[v, k + 2, m] = new
            put_edges(v, k // 2 + 1, 0, m, new)
            terms.append(new * new)
        if k == 0:
            terms.append(old * old)
        return new, tuple(a + tile_sum(b) for a, b in zip(sums, terms))

    def give_back(v, k):
        def body(i, carry):
            to = lax.rem(member + i, GROUP)
            remote(field.at[v, k, to], back.at[k - 1, v, rows_of(block)], sent.at[6], back_sem, base + to).start()
            return carry

        lax.fori_loop(1, GROUP, body, 0)
        pltpu.make_async_copy(field.at[v, k, member], back.at[k - 1, v, rows_of(block)], back_sem).start()

    def partial_faces(v, r):
        for side, (m, inner) in enumerate(((0, 1), (last, last - 1))):
            new = partial(v, 2 * r, m, inner)
            if r < ROUNDS - 1 or side == 1:
                partial_out[v, r, side] = new
            put_edges(v, r, 1, m, new)
        begin(q_copies(v, r))

    def partial_rest(v, r):
        def body(m, carry):
            put_edges(v, r, 1, m, partial(v, 2 * r, m, m - 1, m + 1))
            return carry

        lax.fori_loop(1, last, body, 0, unroll=2)
        begin(y_copies(v, r))

    def arrive(v):
        drain(field.at[v, 0, pl.ds(0, 2)], vec_sem.at[v, 0])
        for z, m in ((0, 0), (1, last)):
            corner_out[v, 0, 2 * z] = field[v, 0, m, 0:1]
            corner_out[v, 0, 2 * z + 1] = field[v, 0, m, rows - 1 : rows]
        begin(z_copies(v, 0))
        drain(field.at[v, 0, pl.ds(1, GROUP - 2)], vec_sem.at[v, 1])
        begin(corner_copies(v, 0))

        def edges(m, carry):
            edge_out[v, 0, 0, 0, m] = field[v, 0, m, 0:1]
            edge_out[v, 0, 1, 0, m] = field[v, 0, m, rows - 1 : rows]
            return carry

        lax.fori_loop(0, GROUP, edges, 0, unroll=True)

    nothing = jnp.zeros((8, lanes), jnp.float32)
    dots = [[None] * (2 * LANCZOS) for v in range(vecs)]

    def advance(v, r):
        k = 2 * r
        final = r == ROUNDS - 1
        weight = 0.5 * scale if k == 0 else scale

        drain(edge_in.at[v, r], edge_sem.at[v, r % 2])

        def complete(m, carry):
            field[v, k + 1, m, 0:8] = field[v, k + 1, m, 0:8] - jnp.where(
                sub == 0, weight * edge_in[v, r, 0, 0, m], 0.0
            )
            field[v, k + 1, m, rows - 8 : rows] = field[v, k + 1, m, rows - 8 : rows] - jnp.where(
                sub == 7, weight * edge_in[v, r, 1, 0, m], 0.0
            )
            return carry

        lax.fori_loop(0, GROUP, complete, 0, unroll=2)
        drain(plane_in.at[v, r], plane_sem.at[v, r % 2])
        for side, m in ((0, 0), (1, last)):
            field[v, k + 1, m] = field[v, k + 1, m] - weight * plane_in[v, r, side]
        if r == 0:
            give_back(v, 1)

        if r in (1, 2):
            give_back(v, r + 1)
        for y in range(2):
            edge[y] = edge_in[v, r, y, 1] - weight * edge_out[v, r, y, 0]

        def outside(side, m):
            here = field[v, k, m] + jnp.concatenate(
                [
                    jnp.where(sub == 0, corner_in[v, r, 2 * side], 0.0),
                    jnp.zeros((rows - 16, lanes), jnp.float32),
                    jnp.where(sub == 7, corner_in[v, r, 2 * side + 1], 0.0),
                ],
                0,
            )
            return partial_in[v, r, side] - weight * here

        def middle(m, sums):
            return follow(v, k, m, field[v, k + 1, m - 1] + field[v, k + 1, m + 1], sums)[1]

        sums = (nothing,) * (3 if final else 5 if k == 0 else 4)
        sums = lax.fori_loop(1, last, middle, sums, unroll=2)
        drain(corner_in.at[v, r], corner_sem.at[v, r % 2])
        for y in range(2):
            for z, m in ((0, 0), (1, last)):
                edge[y, m] = edge[y, m] - weight * corner_in[v, r, 2 * z + y]
        came = partial_in.at[v, r, 0] if final else partial_in.at[v, r]
        if final:
            _, sums = follow(v, k, last, field[v, k + 1, last - 1], sums)
            drain(came, partial_sem.at[v, r % 2])
            _, sums = follow(v, k, 0, field[v, k + 1, 1] + 2.0 * outside(0, 0), sums)
        else:
            drain(came, partial_sem.at[v, r % 2])
            for side, m, inner in ((0, 0, 1), (1, last, last - 1)):
                new, sums = follow(v, k, m, field[v, k + 1, inner] + outside(side, m), sums)
                put_corners(v, r + 1, side, new)
            begin(corner_copies(v, r + 1))
            begin(z_copies(v, r + 1))
            partial_faces(v, r + 1)
            partial_rest(v, r + 1)
        dots[v][2 * k + 1 : 2 * k + 4] = sums[:3]
        if not final:
            dots[v][2 * k + 4] = sums[3]
        if k == 0:
            dots[v][0] = sums[4]

    arrive(0)

    @pl.when(mate)
    def _():
        drain(level.at[others], sent.at[5])
        for v in range(1, vecs):
            scatter_vec(v)

    drain(level, level_sem)
    look_up(0, 0)
    look_up(last, 0)
    for v in range(vecs):
        if v:
            arrive(v)
        partial_faces(v, 0)
        if v == 0:
            lax.fori_loop(1, last, look_up, 0)
        partial_rest(v, 0)
    for r in range(ROUNDS):
        for v in range(vecs):
            advance(v, r)

    lane = lax.broadcasted_iota(jnp.int32, (1, 128), 1)
    tile = jnp.zeros((1, 128), jnp.float32)
    for v in range(vecs):
        for d, value in enumerate(dots[v]):
            whole = jnp.sum(jnp.sum(value, axis=0, keepdims=True), axis=1, keepdims=True)
            tile = jnp.where(lane == v * len(dots[v]) + d, whole, tile)
    mine[...] = tile
    slots[me] = tile

    def tell(i, carry):
        remote(mine, slots.at[me], sum_sem.at[0], sum_sem.at[1], lax.rem(me + i, count)).start()
        return carry

    lax.fori_loop(1, count, tell, 0, unroll=8)
    drain(plane_in, sent.at[0])
    drain(field.at[:, 0, pl.ds(0, 2 * ROUNDS - 1)], sent.at[1])
    drain(edge_out, sent.at[2])
    drain(corner_out, sent.at[3])
    drain(field.at[:, 0, others], sent.at[4])

    @pl.when(jnp.logical_not(mate))
    def _():
        drain(level.at[others], sent.at[5])

    drain(field.at[:, pl.ds(1, RETURNED), others], sent.at[6])
    drain(back, back_sem)
    drain(slots.at[pl.ds(0, count - 1)], sum_sem.at[0])
    drain(slots.at[pl.ds(0, count - 1)], sum_sem.at[1])
    parts = [slots[i] for i in range(count)]
    while len(parts) > 1:
        parts = [a + b for a, b in zip(parts[::2], parts[1::2])] + parts[len(parts) // 2 * 2 :]

    def spread(d):
        at = [v * 2 * LANCZOS + d for v in range(vecs)]
        return jnp.concatenate([jnp.broadcast_to(parts[0][:, i : i + 1], (1, 128)) for i in at], 0)

    nu, diag, offd = lanczos([spread(d) for d in range(2 * LANCZOS)], LANCZOS, jnp.sqrt)
    centre, width = centre[:, :128], width[:, :128]
    diag = [width * a + centre for a in diag]
    offd = [width * b for b in offd]
    third, moments = chebyshev(diag, offd, nu, centre, width)

    at = lax.broadcasted_iota(jnp.int32, small.shape[1:], 1)
    for n, items in enumerate((third, diag, offd, moments)):
        value = jnp.zeros(small.shape[1:], jnp.float32)
        for i, item in enumerate(items):
            value = jnp.where(at == i, item, value)
        small[n] = value


def finish(own, back, small, cheb, diag, offd, moments, mixed, diag_at, offd_at, moments_at, mixed_sem, small_sem):
    vecs, height, lanes = own.shape
    copies = []
    for n, (at, ref) in enumerate(((diag_at, diag), (offd_at, offd), (moments_at, moments))):
        at[...] = small[n + 1, :, : at.shape[1]]
        copies.append(pltpu.make_async_copy(at, ref, small_sem.at[n]))
        copies[-1].start()
    step = height // 2
    third = [
        [jnp.broadcast_to(small[0, v : v + 1, k : k + 1], (1, lanes)) for k in range(RETURNED + 1)] for v in range(vecs)
    ]
    for v in range(vecs):
        for i in range(2):
            part = pl.ds(i * step, step)
            value = third[v][0] * own[v, part]
            for k in range(RETURNED):
                value = value + third[v][k + 1] * back[k, v, part]
            mixed[v, part] = value
            pltpu.make_async_copy(mixed.at[v, part], cheb.at[v, 0, part], mixed_sem).start()
    for copy in copies:
        copy.wait()
    pltpu.make_async_copy(mixed, mixed, mixed_sem).wait()


def shards(count, start_vectors, levels, energies):
    vecs, _, height, lanes = start_vectors.shape
    rows = height // GROUP
    f32 = jnp.float32
    vmem = pl.BlockSpec(memory_space=pltpu.VMEM)
    dma = pltpu.SemaphoreType.DMA
    kept = pl.pallas_call(
        functools.partial(kernel, count),
        out_shape=(
            jax.ShapeDtypeStruct((vecs, height, lanes), f32),
            jax.ShapeDtypeStruct((RETURNED, vecs, height, lanes), f32),
            jax.ShapeDtypeStruct((4, vecs, 128), f32),
        ),
        in_specs=[pl.BlockSpec(memory_space=pltpu.HBM)] * 3,
        out_specs=(vmem,) * 3,
        scratch_shapes=[
            pltpu.SMEM(energies.shape, f32),
            pltpu.VMEM((height, lanes), jnp.int32),
            pltpu.VMEM((vecs, LANCZOS, GROUP, rows, lanes), f32),
            pltpu.VMEM((GROUP, rows, lanes), f32),
            pltpu.VMEM((GROUP, rows, lanes), jnp.int32),
            pltpu.VMEM((vecs, ROUNDS, 2, rows, lanes), f32),
            pltpu.VMEM((vecs, ROUNDS, 2, rows, lanes), f32),
            pltpu.VMEM((vecs, ROUNDS, 2, rows, lanes), f32),
            pltpu.VMEM((vecs, ROUNDS, 2, 2, GROUP, 1, lanes), f32),
            pltpu.VMEM((vecs, ROUNDS, 2, 2, GROUP, 1, lanes), f32),
            pltpu.VMEM((2, GROUP, 1, lanes), f32),
            pltpu.VMEM((vecs, ROUNDS, 4, 1, lanes), f32),
            pltpu.VMEM((vecs, ROUNDS, 4, 1, lanes), f32),
            pltpu.VMEM((count, 1, 128), f32),
            pltpu.VMEM((1, 128), f32),
            dma((vecs + 2,)),
            dma((vecs, 2)),
            dma,
            dma((vecs, 2)),
            dma((vecs, 2)),
            dma((vecs, 2)),
            dma((vecs, 2)),
            dma,
            dma((2,)),
            dma((7,)),
        ],
        compiler_params=pltpu.CompilerParams(
            collective_id=0, has_side_effects=True, vmem_limit_bytes=VMEM_BYTES
        ),
    )(*(pltpu.with_memory_space_constraint(x, pltpu.HBM) for x in (energies, start_vectors, levels)))
    return pl.pallas_call(
        finish,
        out_shape=(
            jax.ShapeDtypeStruct(start_vectors.shape, f32),
            jax.ShapeDtypeStruct((vecs, LANCZOS), f32),
            jax.ShapeDtypeStruct((vecs, LANCZOS - 1), f32),
            jax.ShapeDtypeStruct((vecs, 6), f32),
        ),
        in_specs=[vmem] * 3,
        out_specs=(pl.BlockSpec(memory_space=pltpu.HBM),) * 4,
        scratch_shapes=[
            pltpu.VMEM((vecs, height, lanes), f32),
            pltpu.VMEM((vecs, LANCZOS), f32),
            pltpu.VMEM((vecs, LANCZOS - 1), f32),
            pltpu.VMEM((vecs, 6), f32),
            dma,
            dma((3,)),
        ],
        compiler_params=pltpu.CompilerParams(vmem_limit_bytes=VMEM_BYTES),
    )(*kept)


def solution(mesh):
    in_specs = (P(None, "slab", None, None), P("slab", None, None), P())
    out_specs = (P(None, "slab", None, None), P(), P(), P())
    return jax.shard_map(
        functools.partial(shards, mesh.shape["slab"]),
        mesh=mesh, in_specs=in_specs, out_specs=out_specs, check_vma=False,
    )
```
